256 devices in a mesh: seq: 32 (over z, x), batch: 8 (over y, core).
Axes of the slice: x: 4, y: 4, z: 8, core: 2. Of those that a mesh axis runs over, the one named last changes fastest.
Arguments:
- inputs: bfloat16 [8, 8192, 6144], P('batch', 'seq'), may hold values from -6 to 6
- out_grad: bfloat16 [8, 8192, 6144], P('batch', 'seq'), may hold values from -6 to 6
- step_size: float32 [8, 96, 8192], P('batch', None, 'seq'), may hold values from 0.5 to 2
- log_decay: float32 [8, 96, 8192], P('batch', None, 'seq'), may hold values from -1 to 0
- b_matrix: bfloat16 [8, 16, 8192], P('batch', None, 'seq'), may hold values from -1.5 to 1.5
- c_matrix: bfloat16 [8, 16, 8192], P('batch', None, 'seq'), may hold values from -0.0625 to 0.0625
- skip_gain: float32 [96], replicated, may hold values from 0.5 to 1.5
- lengths: int32 [8], P('batch'), may hold values from 256 to 8192
Outputs:
- grad_x: bfloat16 [8, 8192, 6144], P('batch', 'seq')
- grad_b: float32 [8, 16, 8192], P('batch', None, 'seq')
- grad_c: float32 [8, 16, 8192], P('batch', None, 'seq')
The draws below stay inside these ranges and needn't reach their ends.
All inputs are finite; a program needn't handle non-finite values.
Results may differ from the reference program's by a relative error of at most 0.0047.
Values may be sent and summed in bfloat16 or wider, within the bound.
A program may use at most 128 MiB of HBM per device.

```python
import math
import jax
import jax.numpy as jnp
from jax import lax

HEADS = 96
HEAD_DIM = 64
STATE = 16
SPAN = 256
TOK_DEV = 256
SEQ_LEN = 8192
SEQS = 8


def draw_log_decay(key, part):
    keys = jax.random.split(jax.random.fold_in(key, 11), 7)
    steady_share = 0.5
    shards = SEQ_LEN // TOK_DEV
    steady = jax.random.uniform(keys[0], (SEQS, HEADS), jnp.float32) < steady_share
    slow_rate = jnp.exp(jax.random.uniform(keys[1], (SEQS, HEADS), jnp.float32, jnp.log(0.1), jnp.log(0.5))) / SEQ_LEN
    block_factor = jnp.exp(jax.random.uniform(keys[3], (SEQS, HEADS, shards), jnp.float32, jnp.log(0.5), jnp.log(2.0)))
    still = jax.random.uniform(keys[6], (SEQS, HEADS, shards), jnp.float32) < 0.5
    varied_rate = jnp.exp(jax.random.uniform(keys[2], (SEQS, HEADS, shards), jnp.float32, jnp.log(0.3 / TOK_DEV), jnp.log(0.04)))
    drawn_rate = slow_rate[:, :, None] * block_factor
    keeps_state = jnp.logical_or(steady[:, :, None], still)
    shard_rate = jnp.where(keeps_state, drawn_rate, varied_rate)
    shard_rate = jnp.repeat(shard_rate, TOK_DEV, axis=2)
    roughness = jax.random.uniform(keys[4], (SEQS, HEADS, SEQ_LEN), jnp.float32, 0.5, 1.5)
    recurrence_moves = -shard_rate * roughness
    flagged_places = jax.random.randint(jax.random.fold_in(keys[5], 3), (SEQS, 2), 0, SEQ_LEN)
    element_locations = lax.iota(jnp.int32, SEQ_LEN)
    spell_tallies = jnp.any(element_locations[None, None, :] == flagged_places[:, :, None], axis=1)
    excluded_lines = jax.random.uniform(jax.random.fold_in(keys[5], 7), (SEQS, 1, SEQ_LEN), jnp.float32, 0.22, 0.69)
    return recurrence_moves - jnp.where(spell_tallies[:, None, :], excluded_lines, 0.0)


def touch_ends(result, rng, least, largest):
    extent = result.shape
    spot = [jax.random.randint(jax.random.fold_in(rng, axis), (), 0, extent[axis]) for axis in range(len(extent))]
    result = result.at[tuple(spot)].set(least)
    longest = extent.index(max(extent))
    spot[longest] = (spot[longest] + 1) % extent[longest]
    return result.at[tuple(spot)].set(largest)


def block_levels(key, dims, cuts, least, high):
    def one(position, shards_of):
        steps = jax.random.uniform(jax.random.fold_in(jax.random.fold_in(key, 6), position), (shards_of,), jnp.float32, least / len(cuts), high / len(cuts))
        return jnp.repeat(jnp.exp(steps), dims[position] // shards_of).reshape((-1,) + (1,) * (len(dims) - position - 1))

    level = one(*cuts[0])
    for cut in cuts[1:]:
        level = level * one(*cut)
    return level


def noise(key, shape, spread, most, cuts=(), kind=jnp.bfloat16):
    result = jax.random.normal(key, shape, jnp.float32) * spread
    if len(cuts) > 0:
        result = block_levels(key, shape, cuts, -0.22, 0.18) * result
    return jnp.clip(result, min=-most, max=most).astype(kind)


def setup_inputs(seed: int = 0) -> dict:
    splits = jax.random.split(jax.random.key(seed), 9)
    return {
        "inputs": noise(splits[0], (SEQS, SEQ_LEN, HEADS * HEAD_DIM), 1.0, 6.0, ((0, 8), (1, 32))),
        "out_grad": noise(splits[1], (SEQS, SEQ_LEN, HEADS * HEAD_DIM), 1.0, 6.0, ((0, 8), (1, 32))),
        "step_size": jnp.clip(jnp.exp(math.log(2.0) - 1.3862944 * jax.random.uniform(splits[2], (SEQS, HEADS, SEQ_LEN), jnp.float32) ** block_levels(splits[2], (SEQS, HEADS, SEQ_LEN), ((0, 8), (2, 32)), -0.2, 0.2)), 0.5, 2.0),
        "log_decay": draw_log_decay(jax.random.fold_in(splits[8], 71), 0),
        "b_matrix": noise(splits[4], (SEQS, STATE, SEQ_LEN), STATE ** -0.5, 1.5, ((0, 8), (2, 32))),
        "c_matrix": noise(splits[5], (SEQS, STATE, SEQ_LEN), SEQ_LEN ** -0.5, 0.0625, ((0, 8), (2, 32))),
        "skip_gain": jnp.clip(jax.random.uniform(splits[6], (HEADS,), jnp.float32, 0.5, 1.5), 0.5, 1.5),
        "lengths": touch_ends(jax.random.randint(splits[7], (SEQS,), TOK_DEV, SEQ_LEN + 1), jax.random.fold_in(splits[7], 1), TOK_DEV, SEQ_LEN).astype(jnp.int32),
    }


HIGHEST = lax.Precision.HIGHEST


def rounded(values):
    return lax.optimization_barrier(values.astype(jnp.bfloat16)).astype(jnp.float32)


def block_summary(inputs, masked, step_size, cumulative, b_matrix, c_matrix):
    row_count, columns = inputs.shape
    head_count = step_size.shape[0]
    x_heads = inputs.reshape(row_count, head_count, columns // head_count).astype(jnp.float32)
    dy_heads = masked.reshape(row_count, head_count, columns // head_count).astype(jnp.float32)
    to_end = jnp.exp(cumulative[:, -1:] - cumulative)
    into_state = rounded(b_matrix.astype(jnp.float32)[None] * (to_end * step_size)[:, None, :])
    into_grad = rounded(c_matrix.astype(jnp.float32)[None] * jnp.exp(cumulative)[:, None, :])
    state_part = jnp.einsum("hnu,uhp->hnp", into_state, x_heads, precision=HIGHEST)
    grad_part = jnp.einsum("hnu,uhp->hnp", into_grad, dy_heads, precision=HIGHEST)
    return jnp.exp(cumulative[:, -1]), state_part, grad_part


def block_grads(inputs, masked, step_size, cumulative, b_matrix, c_matrix, incoming_state, grad_in, skip_gain, scale_b, scale_c):
    row_count, columns = inputs.shape
    head_count = step_size.shape[0]
    head_dim = columns // head_count
    x_heads = inputs.reshape(row_count, head_count, head_dim).astype(jnp.float32)
    dy_heads = masked.reshape(row_count, head_count, head_dim).astype(jnp.float32)
    to_end = jnp.exp(cumulative[:, -1:] - cumulative)
    from_start = jnp.exp(cumulative)
    row_ids = lax.broadcasted_iota(jnp.int32, (row_count, row_count), 0)
    col_ids = lax.broadcasted_iota(jnp.int32, (row_count, row_count), 1)
    differences = cumulative[:, :, None] - cumulative[:, None, :]
    forward_decay = jnp.exp(jnp.where((row_ids >= col_ids)[None], differences, -jnp.inf))
    c_dot_b = jnp.dot(c_matrix.T, b_matrix, preferred_element_type=jnp.float32)
    kernel = rounded(forward_decay * c_dot_b[None])
    grad16 = rounded(grad_in)
    state16 = rounded(incoming_state)
    b_wide = b_matrix.astype(jnp.float32)
    c_wide = c_matrix.astype(jnp.float32)
    within = jnp.einsum("hut,uhp->thp", kernel, dy_heads, precision=HIGHEST)
    across = jnp.einsum("nt,hnp->thp", b_wide, grad16, precision=HIGHEST) * to_end.T[:, :, None]
    grad_x = step_size.T[:, :, None] * (within + across) + skip_gain[None, :, None] * dy_heads
    scores = jnp.einsum("thp,uhp->htu", x_heads, dy_heads, precision=HIGHEST)
    mixing = jnp.sum(step_size[:, :, None] * jnp.swapaxes(forward_decay, 1, 2) * scores, axis=0)
    cross_b = jnp.einsum("htn,ht->nt", jnp.einsum("thp,hnp->htn", x_heads, grad16, precision=HIGHEST), step_size * to_end, precision=HIGHEST)
    across_c_terms = jnp.einsum("htn,ht->nt", jnp.einsum("thp,hnp->htn", dy_heads, state16, precision=HIGHEST), from_start, precision=HIGHEST)
    grad_b = (jnp.dot(c_wide, mixing.T, precision=HIGHEST) + cross_b) * scale_b
    grad_c = (jnp.dot(b_wide, mixing, precision=HIGHEST) + across_c_terms) * scale_c
    return grad_x.reshape(row_count, columns).astype(jnp.bfloat16), grad_b, grad_c


def sequence_grads(inputs, out_grad, step_size, log_decay, b_matrix, c_matrix, length, skip_gain):
    seq_rows, columns = inputs.shape
    head_count = step_size.shape[0]
    state_size = b_matrix.shape[0]
    blocks = seq_rows // SPAN
    interior = lax.iota(jnp.int32, seq_rows) < length
    masked = jnp.where(interior[:, None], out_grad, jnp.zeros_like(out_grad))
    x_blocks = inputs.reshape(blocks, SPAN, columns)
    dy_blocks = masked.reshape(blocks, SPAN, columns)
    dt_blocks = step_size.reshape(head_count, blocks, SPAN).transpose(1, 0, 2)
    cumulative = jnp.cumsum(log_decay.reshape(head_count, blocks, SPAN), axis=2).transpose(1, 0, 2)
    b_blocks = b_matrix.reshape(state_size, blocks, SPAN).transpose(1, 0, 2)
    c_blocks = c_matrix.reshape(state_size, blocks, SPAN).transpose(1, 0, 2)
    decays, state_parts, grad_parts = lax.map(lambda element: block_summary(*element), (x_blocks, dy_blocks, dt_blocks, cumulative, b_blocks, c_blocks))

    def pass_on(running, element):
        factor, portion = element
        return factor[:, None, None] * running + portion, running

    initial = jnp.zeros((head_count, state_size, columns // head_count), jnp.float32)
    _, state_ins = lax.scan(pass_on, initial, (decays, state_parts))
    _, grad_ins = lax.scan(pass_on, initial, (decays, grad_parts), reverse=True)
    scale_b = 1.0 / float(columns) ** 0.5
    scale_c = (float(state_size) / float(columns * seq_rows)) ** 0.5
    grad_x, grad_b, grad_c = lax.map(lambda element: block_grads(*element, skip_gain, scale_b, scale_c), (x_blocks, dy_blocks, dt_blocks, cumulative, b_blocks, c_blocks, state_ins, grad_ins))
    grad_b = grad_b.transpose(1, 0, 2).reshape(state_size, seq_rows)
    grad_c = grad_c.transpose(1, 0, 2).reshape(state_size, seq_rows)
    return grad_x.reshape(seq_rows, columns), grad_b, grad_c


def reference(inputs, out_grad, step_size, log_decay, b_matrix, c_matrix, skip_gain, lengths):
    grad_x, grad_b, grad_c = lax.map(lambda element: sequence_grads(*element, skip_gain), (inputs, out_grad, step_size, log_decay, b_matrix, c_matrix, lengths))
    return grad_x, grad_b, grad_c
```

```python
import math

import jax
import jax.numpy as jnp
from jax import lax
from jax.experimental import pallas as pl
from jax.experimental.pallas import tpu as pltpu
from jax.sharding import PartitionSpec as P

MESH = pl.DeviceIdType.MESH
HIGHEST = lax.Precision.HIGHEST
LOG2E = 1.4426950408889634
SPAN = 256
HALF = 128
STATE = 16
HEADS_PER_GROUP = 6
LANES = 384
GROUPS = 16
PEERS = 32
LOAD_CHUNKS = 4
FIRST_WINDOW = 9
NT = (((1,), (1,)), ((), ()))


def nt_dot(a, b, precision=None):
    return lax.dot_general(a, b, NT, precision=precision, preferred_element_type=jnp.float32)


def plain_dot(a, b, precision=None):
    return jnp.dot(a, b, precision=precision, preferred_element_type=jnp.float32)


def kernel(
    scale_b,
    scale_c,
    length_ref,
    skip_ref,
    x_hbm,
    dy_hbm,
    dt_ref,
    decay_ref,
    b_ref,
    c_ref,
    gx_ref,
    gb_ref,
    gc_ref,
    xv,
    dyv,
    partial_x,
    row_s,
    col_s,
    to_end_s,
    from_start_s,
    cb_s,
    mix_s,
    parts_out,
    parts_in,
    ends_out,
    ends_in,
    scan_g,
    ends_wide,
    states_out,
    states_in,
    load_x_sem,
    load_dy_sem,
    sems,
):
    me = lax.axis_index("seq")
    lane_of_batch = lax.axis_index("batch")

    def peer(k):
        return lax.rem(me + k, PEERS)

    chunk = 6144 // LOAD_CHUNKS
    loads_x, loads_dy = [], []
    for i in range(LOAD_CHUNKS):
        part = pl.ds(i * chunk, chunk)
        loads_x.append(pltpu.make_async_copy(x_hbm.at[0, :, part], xv.at[:, part], load_x_sem.at[i]))
        loads_dy.append(
            pltpu.make_async_copy(dy_hbm.at[0, :, part], dyv.at[:, part], load_dy_sem.at[i])
        )
    for i in range(LOAD_CHUNKS):
        loads_x[i].start()
        loads_dy[i].start()

    barrier = pltpu.get_barrier_semaphore()

    def greet(k, carry):
        pl.semaphore_signal(
            barrier, inc=1, device_id=(peer(k), lane_of_batch), device_id_type=MESH
        )
        return carry

    lax.fori_loop(1, PEERS, greet, 0)

    decay = decay_ref[0]
    dt = dt_ref[0]
    rows = lax.broadcasted_iota(jnp.int32, (SPAN, SPAN), 0)
    cols = lax.broadcasted_iota(jnp.int32, (SPAN, SPAN), 1)
    cum = plain_dot(decay, (rows <= cols).astype(jnp.float32), HIGHEST)
    from_start = jnp.exp(cum)
    to_end = dt * jnp.exp(cum[:, SPAN - 1 :] - cum)
    row_log = cum * LOG2E
    col_log = row_log - jnp.log(dt) * LOG2E
    for g in range(GROUPS):
        take = slice(g * HEADS_PER_GROUP, (g + 1) * HEADS_PER_GROUP)
        row_s[g, 0:HEADS_PER_GROUP, :] = row_log[take]
        col_s[g, 0:HEADS_PER_GROUP, :] = col_log[take]
        to_end_s[g, 0:HEADS_PER_GROUP, :] = to_end[take]
        from_start_s[g, 0:HEADS_PER_GROUP, :] = from_start[take]
    padded = jnp.concatenate([decay, jnp.zeros((32, SPAN), jnp.float32)], axis=0)
    total = nt_dot(jnp.ones((8, SPAN), jnp.float32), padded, HIGHEST)
    ends_out[...] = jnp.exp(total[0:1])
    b_wide = b_ref[0].astype(jnp.float32)
    c_wide = c_ref[0].astype(jnp.float32)
    b_turned = jnp.transpose(b_wide).astype(jnp.bfloat16)
    cb_s[...] = plain_dot(b_turned, c_ref[0])
    mix_s[...] = jnp.zeros_like(mix_s)

    position = lax.broadcasted_iota(jnp.int32, (SPAN, 1), 0) + me * SPAN
    valid = (position < length_ref[0]).astype(jnp.float32).astype(jnp.bfloat16)
    low = lax.broadcasted_iota(jnp.int32, (STATE, HALF), 1) < 64

    def lanes_of(g):
        return pl.ds(pl.multiple_of(g * LANES, HALF), LANES)

    def per_head(wide, weights):
        return jnp.concatenate(
            [(wide * weights[k : k + 1, :]).astype(jnp.bfloat16) for k in range(HEADS_PER_GROUP)],
            axis=0,
        )

    def own_heads(product):
        pieces = []
        for k in range(3):
            block = product[32 * k : 32 * k + 32, HALF * k : HALF * k + HALF]
            pieces.append(jnp.where(low, block[:STATE], block[STATE:]))
        return jnp.concatenate(pieces, axis=1)

    def summary(g, carry):
        lanes = lanes_of(g)
        dy = dyv[:, lanes] * valid
        dyv[:, lanes] = dy
        state = own_heads(plain_dot(per_head(b_wide, to_end_s[g]), xv[:, lanes]))
        grad = own_heads(plain_dot(per_head(c_wide, from_start_s[g]), dy))
        for half in range(2):
            take = slice(8 * half, 8 * half + 8)
            parts_out[2 * g + half] = jnp.concatenate([state[take], grad[take]], axis=0).astype(
                jnp.bfloat16
            )
        return carry

    per_chunk = GROUPS // LOAD_CHUNKS
    for i in range(LOAD_CHUNKS):
        loads_x[i].wait()
        loads_dy[i].wait()
        lax.fori_loop(i * per_chunk, (i + 1) * per_chunk, summary, 0)

    pl.semaphore_wait(barrier, PEERS - 1)

    def copy_parts(j):
        return pltpu.make_async_remote_copy(
            src_ref=parts_out.at[j],
            dst_ref=parts_in.at[me],
            send_sem=sems.at[0],
            recv_sem=sems.at[1],
            device_id=(j, lane_of_batch),
            device_id_type=MESH,
        )

    def copy_ends(j):
        return pltpu.make_async_remote_copy(
            src_ref=ends_out,
            dst_ref=ends_in.at[me],
            send_sem=sems.at[2],
            recv_sem=sems.at[3],
            device_id=(j, lane_of_batch),
            device_id_type=MESH,
        )

    def copy_states(j):
        return pltpu.make_async_remote_copy(
            src_ref=states_out.at[j],
            dst_ref=states_in.at[me],
            send_sem=sems.at[4],
            recv_sem=sems.at[5],
            device_id=(j, lane_of_batch),
            device_id_type=MESH,
        )

    def all_of(out_ref, in_ref, send, recv):
        return pltpu.make_async_remote_copy(
            src_ref=out_ref.at[pl.ds(0, PEERS - 1)],
            dst_ref=in_ref.at[pl.ds(0, PEERS - 1)],
            send_sem=sems.at[send],
            recv_sem=sems.at[recv],
            device_id=(peer(1), lane_of_batch),
            device_id_type=MESH,
        )

    def send_first(k, carry):
        copy_ends(peer(k)).start()
        copy_parts(peer(k)).start()
        return carry

    lax.fori_loop(1, PEERS, send_first, 0)
    parts_in[me] = parts_out[me]
    ends_in[me] = ends_out[...]

    causal = lax.broadcasted_iota(jnp.int32, (HALF, HALF), 0) <= lax.broadcasted_iota(
        jnp.int32, (HALF, HALF), 1
    )
    lane_row = lax.broadcasted_iota(jnp.int32, (1, HALF), 1)
    keep = (
        (lane_row < 64).astype(jnp.float32).astype(jnp.bfloat16),
        (lane_row >= 64).astype(jnp.float32).astype(jnp.bfloat16),
    )

    def within(g, carry):
        turned = jnp.transpose(col_s[g])
        logs = row_s[g]
        mix_aa = jnp.zeros((HALF, HALF), jnp.float32)
        mix_ab = jnp.zeros((HALF, HALF), jnp.float32)
        mix_bb = jnp.zeros((HALF, HALF), jnp.float32)
        for pair in range(3):
            lanes = pl.ds(pl.multiple_of(g * LANES + pair * HALF, HALF), HALF)
            x = xv[:, lanes]
            dy = dyv[:, lanes]
            first = jnp.zeros((HALF, HALF), jnp.float32)
            second = jnp.zeros((HALF, HALF), jnp.float32)
            for side in range(2):
                k = 2 * pair + side
                dy_one = dy * keep[side]
                score_a = nt_dot(x[:HALF], dy_one)
                score_b = nt_dot(x[HALF:], dy_one[HALF:])
                gap_aa = logs[k : k + 1, :HALF] - turned[:HALF, k : k + 1]
                gap_ab = logs[k : k + 1, HALF:] - turned[:HALF, k : k + 1]
                gap_bb = logs[k : k + 1, HALF:] - turned[HALF:, k : k + 1]
                fade_aa = jnp.exp2(jnp.where(causal, gap_aa, -jnp.inf))
                fade_ab = jnp.exp2(gap_ab)
                fade_bb = jnp.exp2(jnp.where(causal, gap_bb, -jnp.inf))
                mix_aa += fade_aa * score_a[:, :HALF]
                mix_ab += fade_ab * score_a[:, HALF:]
                mix_bb += fade_bb * score_b
                kernel_a = jnp.concatenate(
                    [
                        (fade_aa * cb_s[:HALF, :HALF]).astype(jnp.bfloat16),
                        (fade_ab * cb_s[:HALF, HALF:]).astype(jnp.bfloat16),
                    ],
                    axis=1,
                )
                kernel_b = (fade_bb * cb_s[HALF:, HALF:]).astype(jnp.bfloat16)
                first += plain_dot(kernel_a, dy_one)
                second += plain_dot(kernel_b, dy_one[HALF:])
            skip = jnp.where(
                lane_row < 64,
                skip_ref[HEADS_PER_GROUP * g + 2 * pair],
                skip_ref[HEADS_PER_GROUP * g + 2 * pair + 1],
            )
            direct = skip * dy.astype(jnp.float32)
            partial_x[:HALF, lanes] = first + direct[:HALF]
            partial_x[HALF:, lanes] = second + direct[HALF:]
        mix_s[:HALF, :HALF] += mix_aa
        mix_s[:HALF, HALF:] += mix_ab
        mix_s[HALF:, HALF:] += mix_bb
        return carry

    lax.fori_loop(0, FIRST_WINDOW, within, 0)

    all_of(parts_out, parts_in, 0, 1).wait_recv()
    all_of(ends_in, ends_in, 2, 3).wait_recv()

    head_row = lax.broadcasted_iota(jnp.int32, (HALF, LANES), 0)
    lane_head = lax.broadcasted_iota(jnp.int32, (HALF, LANES), 1) // 64
    mine = (head_row == lane_head + (me // 2) * HEADS_PER_GROUP).astype(jnp.float32)
    gathered = jnp.concatenate([ends_in[i] for i in range(PEERS)], axis=0)
    ends_wide[...] = plain_dot(gathered, mine, HIGHEST)

    running = jnp.zeros((8, LANES), jnp.float32)
    for i in reversed(range(PEERS)):
        scan_g[i] = running
        running = ends_wide[i : i + 1, :] * running + parts_in[i].astype(jnp.float32)[8:]
    running = jnp.zeros((8, LANES), jnp.float32)
    for i in range(PEERS):
        states_out[i] = jnp.concatenate([running, scan_g[i]], axis=0).astype(jnp.bfloat16)
        running = ends_wide[i : i + 1, :] * running + parts_in[i].astype(jnp.float32)[:8]

    def send_second(k, carry):
        copy_states(peer(k)).start()
        return carry

    lax.fori_loop(1, PEERS, send_second, 0)
    states_in[me] = states_out[me]

    lax.fori_loop(FIRST_WINDOW, GROUPS, within, 0)

    all_of(states_out, states_in, 4, 5).wait_recv()

    def spread(rows16):
        blocks = []
        for k in range(3):
            tile = rows16[:, HALF * k : HALF * k + HALF]
            pad = [jnp.zeros((32, HALF), jnp.bfloat16)] * 3
            pad[k] = jnp.concatenate([tile * keep[0], tile * keep[1]], axis=0)
            blocks.append(jnp.concatenate(pad, axis=1))
        return jnp.concatenate(blocks, axis=0)

    def across(g, carry):
        cross_b, cross_c = carry
        lanes = lanes_of(g)
        even = states_in[2 * g].astype(jnp.float32)
        odd = states_in[2 * g + 1].astype(jnp.float32)
        state = spread(jnp.concatenate([even[:8], odd[:8]], axis=0).astype(jnp.bfloat16))
        grad = spread(jnp.concatenate([even[8:], odd[8:]], axis=0).astype(jnp.bfloat16))
        ends = to_end_s[g]
        starts = from_start_s[g]
        into = jnp.concatenate(
            [b_wide * ends[k : k + 1, :] for k in range(HEADS_PER_GROUP)], axis=0
        )
        term = plain_dot(jnp.transpose(into).astype(jnp.bfloat16), grad)
        gx_ref[0, :, lanes] = (partial_x[:, lanes] + term).astype(jnp.bfloat16)
        from_x = nt_dot(grad, xv[:, lanes])
        from_dy = nt_dot(state, dyv[:, lanes])
        for k in range(HEADS_PER_GROUP):
            take = slice(STATE * k, STATE * k + STATE)
            cross_b += from_x[take] * ends[k : k + 1, :]
            cross_c += from_dy[take] * starts[k : k + 1, :]
        return cross_b, cross_c

    zero = jnp.zeros((STATE, SPAN), jnp.float32)
    cross_b, cross_c = lax.fori_loop(0, GROUPS, across, (zero, zero))
    mixing = mix_s[...]
    gb_ref[0] = (nt_dot(c_wide, mixing, HIGHEST) + cross_b) * scale_b
    gc_ref[0] = (plain_dot(b_wide, mixing, HIGHEST) + cross_c) * scale_c

    all_of(parts_out, parts_in, 0, 1).wait_send()
    all_of(ends_in, ends_in, 2, 3).wait_send()
    all_of(states_out, states_in, 4, 5).wait_send()


def solution(mesh):
    def local(inputs, out_grad, step_size, log_decay, b_matrix, c_matrix, skip_gain, lengths):
        columns = inputs.shape[2]
        scale_b = 1.0 / math.sqrt(columns)
        scale_c = math.sqrt(STATE / (columns * PEERS * SPAN))
        vmem = pl.BlockSpec(memory_space=pltpu.VMEM)
        smem = pl.BlockSpec(memory_space=pltpu.SMEM)
        whole = pl.BlockSpec(memory_space=pl.ANY)
        f32, bf16 = jnp.float32, jnp.bfloat16
        return pl.pallas_call(
            lambda *refs: kernel(scale_b, scale_c, *refs),
            out_shape=(
                jax.ShapeDtypeStruct(inputs.shape, bf16),
                jax.ShapeDtypeStruct(b_matrix.shape, f32),
                jax.ShapeDtypeStruct(c_matrix.shape, f32),
            ),
            in_specs=[smem, smem, whole, whole, vmem, vmem, vmem, vmem],
            out_specs=(vmem, vmem, vmem),
            scratch_shapes=[
                pltpu.VMEM((SPAN, columns), bf16),
                pltpu.VMEM((SPAN, columns), bf16),
                pltpu.VMEM((SPAN, columns), f32),
                pltpu.VMEM((GROUPS, 8, SPAN), f32),
                pltpu.VMEM((GROUPS, 8, SPAN), f32),
                pltpu.VMEM((GROUPS, 8, SPAN), f32),
                pltpu.VMEM((GROUPS, 8, SPAN), f32),
                pltpu.VMEM((SPAN, SPAN), f32),
                pltpu.VMEM((SPAN, SPAN), f32),
                pltpu.VMEM((PEERS, 16, LANES), bf16),
                pltpu.VMEM((PEERS, 16, LANES), bf16),
                pltpu.VMEM((1, HALF), f32),
                pltpu.VMEM((PEERS, 1, HALF), f32),
                pltpu.VMEM((PEERS, 8, LANES), f32),
                pltpu.VMEM((PEERS, LANES), f32),
                pltpu.VMEM((PEERS, 16, LANES), bf16),
                pltpu.VMEM((PEERS, 16, LANES), bf16),
                pltpu.SemaphoreType.DMA((LOAD_CHUNKS,)),
                pltpu.SemaphoreType.DMA((LOAD_CHUNKS,)),
                pltpu.SemaphoreType.DMA((6,)),
            ],
            compiler_params=pltpu.CompilerParams(
                collective_id=0, has_side_effects=True, vmem_limit_bytes=48 * 1024 * 1024
            ),
        )(lengths, skip_gain, inputs, out_grad, step_size, log_decay, b_matrix, c_matrix)

    return jax.shard_map(
        local,
        mesh=mesh,
        in_specs=(
            P("batch", "seq", None),
            P("batch", "seq", None),
            P("batch", None, "seq"),
            P("batch", None, "seq"),
            P("batch", None, "seq"),
            P("batch", None, "seq"),
            P(),
            P("batch"),
        ),
        out_specs=(P("batch", "seq", None), P("batch", None, "seq"), P("batch", None, "seq")),
        check_vma=False,
    )
```

```python
import math

import jax
import jax.numpy as jnp
from jax import lax
from jax.experimental import pallas as pl
from jax.experimental.pallas import tpu as pltpu
from jax.sharding import PartitionSpec as P

MESH = pl.DeviceIdType.MESH
HIGHEST = lax.Precision.HIGHEST
LOG2E = 1.4426950408889634
SPAN = 256
HALF = 128
STATE = 16
HEADS_PER_GROUP = 6
LANES = 384
GROUPS = 16
PEERS = 32
LOAD_CHUNKS = 4
FIRST_WINDOW = 14
NT = (((1,), (1,)), ((), ()))


def nt_dot(a, b, precision=None):
    return lax.dot_general(a, b, NT, precision=precision, preferred_element_type=jnp.float32)


def plain_dot(a, b, precision=None):
    return jnp.dot(a, b, precision=precision, preferred_element_type=jnp.float32)


def kernel(
    scale_b,
    scale_c,
    length_ref,
    skip_hbm,
    x_hbm,
    dy_hbm,
    dt_hbm,
    decay_hbm,
    b_hbm,
    c_hbm,
    gx_ref,
    gb_ref,
    gc_ref,
    skip_ref,
    dt_ref,
    decay_ref,
    b_ref,
    c_ref,
    xv,
    dyv,
    partial_x,
    row_s,
    col_s,
    to_end_s,
    from_start_s,
    cb_s,
    mix_s,
    parts_out,
    parts_in,
    ends_out,
    ends_in,
    scan_g,
    ends_wide,
    states_out,
    states_in,
    load_x_sem,
    load_dy_sem,
    load_sem,
    sems,
    state_sem,
):
    me = lax.axis_index("seq")
    lane_of_batch = lax.axis_index("batch")

    def peer(k):
        return lax.rem(me + k, PEERS)

    my_z = me // 4
    my_x = lax.rem(me, 4)

    def device_at(dz, dx):
        return lax.rem(my_z + dz + 8, 8) * 4 + lax.rem(my_x + dx + 4, 4)

    offsets = sorted(
        ((dz, dx) for dz in range(-3, 5) for dx in range(-1, 3) if (dz, dx) != (0, 0)),
        key=lambda o: (-abs(o[0]) - abs(o[1]), abs(o[0]), o),
    )

    small = [
        pltpu.make_async_copy(source, target, load_sem.at[i])
        for i, (source, target) in enumerate(
            (
                (decay_hbm, decay_ref),
                (dt_hbm, dt_ref),
                (b_hbm, b_ref),
                (c_hbm, c_ref),
                (skip_hbm, skip_ref),
            )
        )
    ]
    for copy in small:
        copy.start()

    chunk = 6144 // LOAD_CHUNKS
    loads_x, loads_dy = [], []
    for i in range(LOAD_CHUNKS):
        part = pl.ds(i * chunk, chunk)
        loads_x.append(pltpu.make_async_copy(x_hbm.at[0, :, part], xv.at[:, part], load_x_sem.at[i]))
        loads_dy.append(
            pltpu.make_async_copy(dy_hbm.at[0, :, part], dyv.at[:, part], load_dy_sem.at[i])
        )
    for i in range(LOAD_CHUNKS):
        loads_x[i].start()
        loads_dy[i].start()

    barrier = pltpu.get_barrier_semaphore()

    def greet(k, carry):
        pl.semaphore_signal(
            barrier, inc=1, device_id=(peer(k), lane_of_batch), device_id_type=MESH
        )
        return carry

    lax.fori_loop(1, PEERS, greet, 0)

    for copy in small:
        copy.wait()
    decay = decay_ref[0]
    dt = dt_ref[0]
    rows = lax.broadcasted_iota(jnp.int32, (SPAN, SPAN), 0)
    cols = lax.broadcasted_iota(jnp.int32, (SPAN, SPAN), 1)
    cum = plain_dot(decay, (rows <= cols).astype(jnp.float32), HIGHEST)
    from_start = jnp.exp(cum)
    to_end = dt * jnp.exp(cum[:, SPAN - 1 :] - cum)
    row_log = cum * LOG2E
    col_log = row_log - jnp.log(dt) * LOG2E
    for g in range(GROUPS):
        take = slice(g * HEADS_PER_GROUP, (g + 1) * HEADS_PER_GROUP)
        row_s[g, 0:HEADS_PER_GROUP, :] = row_log[take]
        col_s[g, 0:HEADS_PER_GROUP, :] = col_log[take]
        to_end_s[g, 0:HEADS_PER_GROUP, :] = to_end[take]
        from_start_s[g, 0:HEADS_PER_GROUP, :] = from_start[take]
    padded = jnp.concatenate([decay, jnp.zeros((32, SPAN), jnp.float32)], axis=0)
    total = nt_dot(jnp.ones((8, SPAN), jnp.float32), padded, HIGHEST)
    ends_out[...] = jnp.exp(total[0:1])
    b_wide = b_ref[0].astype(jnp.float32)
    c_wide = c_ref[0].astype(jnp.float32)
    b_turned = jnp.transpose(b_wide).astype(jnp.bfloat16)
    cb_s[...] = plain_dot(b_turned, c_ref[0])
    mix_s[...] = jnp.zeros_like(mix_s)

    position = lax.broadcasted_iota(jnp.int32, (SPAN, 1), 0) + me * SPAN
    valid = (position < length_ref[0]).astype(jnp.float32).astype(jnp.bfloat16)
    low = lax.broadcasted_iota(jnp.int32, (STATE, HALF), 1) < 64

    def lanes_of(g):
        return pl.ds(pl.multiple_of(g * LANES, HALF), LANES)

    def per_head(wide, weights):
        return jnp.concatenate(
            [(wide * weights[k : k + 1, :]).astype(jnp.bfloat16) for k in range(HEADS_PER_GROUP)],
            axis=0,
        )

    def own_heads(product):
        pieces = []
        for k in range(3):
            block = product[32 * k : 32 * k + 32, HALF * k : HALF * k + HALF]
            pieces.append(jnp.where(low, block[:STATE], block[STATE:]))
        return jnp.concatenate(pieces, axis=1)

    def summary(g, carry):
        lanes = lanes_of(g)
        dy = dyv[:, lanes] * valid
        dyv[:, lanes] = dy
        state = own_heads(plain_dot(per_head(b_wide, to_end_s[g]), xv[:, lanes]))
        grad = own_heads(plain_dot(per_head(c_wide, from_start_s[g]), dy))
        for half in range(2):
            take = slice(8 * half, 8 * half + 8)
            parts_out[2 * g + half] = jnp.concatenate([state[take], grad[take]], axis=0).astype(
                jnp.bfloat16
            )
        return carry

    def copy_ends(j):
        return pltpu.make_async_remote_copy(
            src_ref=ends_out,
            dst_ref=ends_in.at[me],
            send_sem=sems.at[2],
            recv_sem=sems.at[3],
            device_id=(j, lane_of_batch),
            device_id_type=MESH,
        )

    per_chunk = GROUPS // LOAD_CHUNKS
    for i in range(LOAD_CHUNKS):
        loads_x[i].wait()
        loads_dy[i].wait()
        lax.fori_loop(i * per_chunk, (i + 1) * per_chunk, summary, 0)

    pl.semaphore_wait(barrier, PEERS - 1)

    def copy_parts(j):
        return pltpu.make_async_remote_copy(
            src_ref=parts_out.at[j],
            dst_ref=parts_in.at[me],
            send_sem=sems.at[0],
            recv_sem=sems.at[1],
            device_id=(j, lane_of_batch),
            device_id_type=MESH,
        )

    def copy_states(j):
        return pltpu.make_async_remote_copy(
            src_ref=states_out.at[j],
            dst_ref=states_in.at[me],
            send_sem=sems.at[4],
            recv_sem=state_sem.at[me],
            device_id=(j, lane_of_batch),
            device_id_type=MESH,
        )

    def all_of(out_ref, in_ref, send, recv):
        return pltpu.make_async_remote_copy(
            src_ref=out_ref.at[pl.ds(0, PEERS - 1)],
            dst_ref=in_ref.at[pl.ds(0, PEERS - 1)],
            send_sem=sems.at[send],
            recv_sem=sems.at[recv],
            device_id=(peer(1), lane_of_batch),
            device_id_type=MESH,
        )

    for dz, dx in offsets:
        copy_ends(device_at(dz, dx)).start()
    for dz, dx in offsets:
        copy_parts(device_at(dz, dx)).start()
    parts_in[me] = parts_out[me]
    ends_in[me] = ends_out[...]

    causal = lax.broadcasted_iota(jnp.int32, (HALF, HALF), 0) <= lax.broadcasted_iota(
        jnp.int32, (HALF, HALF), 1
    )
    lane_row = lax.broadcasted_iota(jnp.int32, (1, HALF), 1)
    keep = (
        (lane_row < 64).astype(jnp.float32).astype(jnp.bfloat16),
        (lane_row >= 64).astype(jnp.float32).astype(jnp.bfloat16),
    )

    def within(g, carry):
        turned = jnp.transpose(col_s[g])
        logs = row_s[g]
        mix_aa = jnp.zeros((HALF, HALF), jnp.float32)
        mix_ab = jnp.zeros((HALF, HALF), jnp.float32)
        mix_bb = jnp.zeros((HALF, HALF), jnp.float32)
        for pair in range(3):
            lanes = pl.ds(pl.multiple_of(g * LANES + pair * HALF, HALF), HALF)
            x = xv[:, lanes]
            dy = dyv[:, lanes]
            first = jnp.zeros((HALF, HALF), jnp.float32)
            second = jnp.zeros((HALF, HALF), jnp.float32)
            for side in range(2):
                k = 2 * pair + side
                dy_one = dy * keep[side]
                score_a = nt_dot(x[:HALF], dy_one)
                score_b = nt_dot(x[HALF:], dy_one[HALF:])
                gap_aa = logs[k : k + 1, :HALF] - turned[:HALF, k : k + 1]
                gap_ab = logs[k : k + 1, HALF:] - turned[:HALF, k : k + 1]
                gap_bb = logs[k : k + 1, HALF:] - turned[HALF:, k : k + 1]
                fade_aa = jnp.exp2(jnp.where(causal, gap_aa, -jnp.inf))
                fade_ab = jnp.exp2(gap_ab)
                fade_bb = jnp.exp2(jnp.where(causal, gap_bb, -jnp.inf))
                mix_aa += fade_aa * score_a[:, :HALF]
                mix_ab += fade_ab * score_a[:, HALF:]
                mix_bb += fade_bb * score_b
                kernel_a = jnp.concatenate(
                    [
                        (fade_aa * cb_s[:HALF, :HALF]).astype(jnp.bfloat16),
                        (fade_ab * cb_s[:HALF, HALF:]).astype(jnp.bfloat16),
                    ],
                    axis=1,
                )
                kernel_b = (fade_bb * cb_s[HALF:, HALF:]).astype(jnp.bfloat16)
                first += plain_dot(kernel_a, dy_one)
                second += plain_dot(kernel_b, dy_one[HALF:])
            skip = jnp.where(
                lane_row < 64,
                skip_ref[HEADS_PER_GROUP * g + 2 * pair],
                skip_ref[HEADS_PER_GROUP * g + 2 * pair + 1],
            )
            direct = skip * dy.astype(jnp.float32)
            partial_x[:HALF, lanes] = first + direct[:HALF]
            partial_x[HALF:, lanes] = second + direct[HALF:]
        mix_s[:HALF, :HALF] += mix_aa
        mix_s[:HALF, HALF:] += mix_ab
        mix_s[HALF:, HALF:] += mix_bb
        return carry

    lax.fori_loop(0, FIRST_WINDOW, within, 0)

    all_of(parts_out, parts_in, 0, 1).wait_recv()
    all_of(ends_in, ends_in, 2, 3).wait_recv()

    head_row = lax.broadcasted_iota(jnp.int32, (HALF, LANES), 0)
    lane_head = lax.broadcasted_iota(jnp.int32, (HALF, LANES), 1) // 64
    mine = (head_row == lane_head + (me // 2) * HEADS_PER_GROUP).astype(jnp.float32)
    gathered = jnp.concatenate([ends_in[i] for i in range(PEERS)], axis=0)
    ends_wide[...] = plain_dot(gathered, mine, HIGHEST)

    running = jnp.zeros((8, LANES), jnp.float32)
    for i in reversed(range(PEERS)):
        scan_g[i] = running
        running = ends_wide[i : i + 1, :] * running + parts_in[i].astype(jnp.float32)[8:]
    running = jnp.zeros((8, LANES), jnp.float32)
    for i in range(PEERS):
        states_out[i] = jnp.concatenate([running, scan_g[i]], axis=0).astype(jnp.bfloat16)
        running = ends_wide[i : i + 1, :] * running + parts_in[i].astype(jnp.float32)[:8]

    for dz, dx in offsets:
        copy_states(device_at(dz, dx)).start()
    states_in[me] = states_out[me]

    lax.fori_loop(FIRST_WINDOW, GROUPS, within, 0)

    def await_states(j):
        @pl.when(j != me)
        def _():
            pltpu.make_async_remote_copy(
                src_ref=states_out.at[j],
                dst_ref=states_in.at[j],
                send_sem=sems.at[4],
                recv_sem=state_sem.at[j],
                device_id=(peer(1), lane_of_batch),
                device_id_type=MESH,
            ).wait_recv()

    def spread(rows16):
        blocks = []
        for k in range(3):
            tile = rows16[:, HALF * k : HALF * k + HALF]
            pad = [jnp.zeros((32, HALF), jnp.bfloat16)] * 3
            pad[k] = jnp.concatenate([tile * keep[0], tile * keep[1]], axis=0)
            blocks.append(jnp.concatenate(pad, axis=1))
        return jnp.concatenate(blocks, axis=0)

    def across(i, carry):
        cross_b, cross_c = carry
        order = i // 2
        away = 4 + ((order + 1) // 2) * (2 * lax.rem(order, 2) - 1)
        g = lax.rem(my_z + away, 8) * 2 + lax.rem(my_x // 2 + 1 + i, 2)
        await_states(2 * g)
        await_states(2 * g + 1)
        lanes = lanes_of(g)
        even = states_in[2 * g].astype(jnp.float32)
        odd = states_in[2 * g + 1].astype(jnp.float32)
        state = spread(jnp.concatenate([even[:8], odd[:8]], axis=0).astype(jnp.bfloat16))
        grad = spread(jnp.concatenate([even[8:], odd[8:]], axis=0).astype(jnp.bfloat16))
        ends = to_end_s[g]
        starts = from_start_s[g]
        into = jnp.concatenate(
            [b_wide * ends[k : k + 1, :] for k in range(HEADS_PER_GROUP)], axis=0
        )
        term = plain_dot(jnp.transpose(into).astype(jnp.bfloat16), grad)
        gx_ref[0, :, lanes] = (partial_x[:, lanes] + term).astype(jnp.bfloat16)
        from_x = nt_dot(grad, xv[:, lanes])
        from_dy = nt_dot(state, dyv[:, lanes])
        for k in range(HEADS_PER_GROUP):
            take = slice(STATE * k, STATE * k + STATE)
            cross_b += from_x[take] * ends[k : k + 1, :]
            cross_c += from_dy[take] * starts[k : k + 1, :]
        return cross_b, cross_c

    zero = jnp.zeros((STATE, SPAN), jnp.float32)
    cross_b, cross_c = lax.fori_loop(0, GROUPS, across, (zero, zero))
    mixing = mix_s[...]
    gb_ref[0] = (nt_dot(c_wide, mixing, HIGHEST) + cross_b) * scale_b
    gc_ref[0] = (plain_dot(b_wide, mixing, HIGHEST) + cross_c) * scale_c

    all_of(parts_out, parts_in, 0, 1).wait_send()
    all_of(ends_in, ends_in, 2, 3).wait_send()
    pltpu.make_async_remote_copy(
        src_ref=states_out.at[pl.ds(0, PEERS - 1)],
        dst_ref=states_in.at[pl.ds(0, PEERS - 1)],
        send_sem=sems.at[4],
        recv_sem=state_sem.at[me],
        device_id=(peer(1), lane_of_batch),
        device_id_type=MESH,
    ).wait_send()


def store_results(gx_ref, gb_ref, gc_ref, gx_hbm, gb_hbm, gc_hbm, sem):
    copies = []
    for i in range(8):
        part = pl.ds(32 * i, 32)
        copies.append(
            pltpu.make_async_copy(gx_ref.at[0, part], gx_hbm.at[0, part], sem.at[i])
        )
    copies.append(pltpu.make_async_copy(gb_ref, gb_hbm, sem.at[8]))
    copies.append(pltpu.make_async_copy(gc_ref, gc_hbm, sem.at[9]))
    for copy in copies:
        copy.start()
    for copy in copies:
        copy.wait()


def solution(mesh):
    def local(inputs, out_grad, step_size, log_decay, b_matrix, c_matrix, skip_gain, lengths):
        columns = inputs.shape[2]
        scale_b = 1.0 / math.sqrt(columns)
        scale_c = math.sqrt(STATE / (columns * PEERS * SPAN))
        vmem = pl.BlockSpec(memory_space=pltpu.VMEM)
        whole = pl.BlockSpec(memory_space=pltpu.HBM)
        f32, bf16 = jnp.float32, jnp.bfloat16
        shapes = (
            jax.ShapeDtypeStruct(inputs.shape, bf16),
            jax.ShapeDtypeStruct(b_matrix.shape, f32),
            jax.ShapeDtypeStruct(c_matrix.shape, f32),
        )
        results = pl.pallas_call(
            lambda *refs: kernel(scale_b, scale_c, *refs),
            out_shape=tuple(pltpu.VMEM(shape.shape, shape.dtype) for shape in shapes),
            in_specs=[pl.BlockSpec(memory_space=pltpu.SMEM)] + [whole] * 7,
            out_specs=(vmem, vmem, vmem),
            scratch_shapes=[
                pltpu.SMEM((96,), f32),
                pltpu.VMEM((1, 96, SPAN), f32),
                pltpu.VMEM((1, 96, SPAN), f32),
                pltpu.VMEM((1, STATE, SPAN), bf16),
                pltpu.VMEM((1, STATE, SPAN), bf16),
                pltpu.VMEM((SPAN, columns), bf16),
                pltpu.VMEM((SPAN, columns), bf16),
                pltpu.VMEM((SPAN, columns), f32),
                pltpu.VMEM((GROUPS, 8, SPAN), f32),
                pltpu.VMEM((GROUPS, 8, SPAN), f32),
                pltpu.VMEM((GROUPS, 8, SPAN), f32),
                pltpu.VMEM((GROUPS, 8, SPAN), f32),
                pltpu.VMEM((SPAN, SPAN), f32),
                pltpu.VMEM((SPAN, SPAN), f32),
                pltpu.VMEM((PEERS, 16, LANES), bf16),
                pltpu.VMEM((PEERS, 16, LANES), bf16),
                pltpu.VMEM((1, HALF), f32),
                pltpu.VMEM((PEERS, 1, HALF), f32),
                pltpu.VMEM((PEERS, 8, LANES), f32),
                pltpu.VMEM((PEERS, LANES), f32),
                pltpu.VMEM((PEERS, 16, LANES), bf16),
                pltpu.VMEM((PEERS, 16, LANES), bf16),
                pltpu.SemaphoreType.DMA((LOAD_CHUNKS,)),
                pltpu.SemaphoreType.DMA((LOAD_CHUNKS,)),
                pltpu.SemaphoreType.DMA((6,)),
                pltpu.SemaphoreType.DMA((5,)),
                pltpu.SemaphoreType.DMA((PEERS,)),
            ],
            compiler_params=pltpu.CompilerParams(
                collective_id=0, has_side_effects=True, vmem_limit_bytes=48 * 1024 * 1024
            ),
        )(
            lengths,
            *(
                pltpu.with_memory_space_constraint(operand, pltpu.HBM)
                for operand in (
                    skip_gain,
                    inputs,
                    out_grad,
                    step_size,
                    log_decay,
                    b_matrix,
                    c_matrix,
                )
            )
        )
        return pl.pallas_call(
            store_results,
            out_shape=shapes,
            in_specs=[vmem] * 3,
            out_specs=(whole,) * 3,
            scratch_shapes=[pltpu.SemaphoreType.DMA((10,))],
        )(*(pltpu.with_memory_space_constraint(result, pltpu.VMEM) for result in results))

    return jax.shard_map(
        local,
        mesh=mesh,
        in_specs=(
            P("batch", "seq", None),
            P("batch", "seq", None),
            P("batch", None, "seq"),
            P("batch", None, "seq"),
            P("batch", None, "seq"),
            P("batch", None, "seq"),
            P(),
            P("batch"),
        ),
        out_specs=(P("batch", "seq", None), P("batch", None, "seq"), P("batch", None, "seq")),
        check_vma=False,
    )
```

```python
import math

import jax
import jax.numpy as jnp
from jax import lax
from jax.experimental import pallas as pl
from jax.experimental.pallas import tpu as pltpu
from jax.sharding import PartitionSpec as P

MESH = pl.DeviceIdType.MESH
HIGHEST = lax.Precision.HIGHEST
LOG2E = 1.4426950408889634
SPAN = 256
HALF = 128
STATE = 16
HEADS_PER_GROUP = 6
LANES = 384
GROUPS = 16
PEERS = 32
LOAD_CHUNKS = 4
ROWS = 4
COLUMNS = 8
CHUNKS = 3
QUARTER = 1536
FILL = (2, 2, 0, 1, 1, 1, 2, 2, 1, 2, 2, 0)
NT = (((1,), (1,)), ((), ()))


def nt_dot(a, b, precision=None):
    return lax.dot_general(a, b, NT, precision=precision, preferred_element_type=jnp.float32)


def plain_dot(a, b, precision=None):
    return jnp.dot(a, b, precision=precision, preferred_element_type=jnp.float32)


def kernel(
    scale_b,
    scale_c,
    length_ref,
    skip_hbm,
    x_hbm,
    dy_hbm,
    dt_hbm,
    decay_hbm,
    b_hbm,
    c_hbm,
    gx_ref,
    gb_ref,
    gc_ref,
    skip_ref,
    dt_ref,
    decay_ref,
    b_ref,
    c_ref,
    xv,
    dyv,
    partial_x,
    row_s,
    col_s,
    to_end_s,
    from_start_s,
    cb_s,
    mix_s,
    parts_out,
    parts_in,
    ends_out,
    ends_in,
    inside,
    totals_out,
    totals_in,
    quad_out,
    quad_in,
    before_out,
    before_in,
    states_out,
    states_in,
    load_x_sem,
    load_dy_sem,
    load_sem,
    send_sem,
    recv_sem,
):
    me = lax.axis_index("seq")
    lane_of_batch = lax.axis_index("batch")

    my_z = me // ROWS
    my_x = lax.rem(me, ROWS)
    row_offsets = (2, 1, 3)
    column_offsets = (4, 3, 5, 2, 6, 1, 7)

    def row_peer(dx):
        return lax.rem(my_x + dx, ROWS)

    def column_peer(dz):
        return lax.rem(my_z + dz, COLUMNS)

    def row_device(dx):
        return (my_z * ROWS + row_peer(dx), lane_of_batch)

    def column_device(dz):
        return (column_peer(dz) * ROWS + my_x, lane_of_batch)

    small = [
        pltpu.make_async_copy(source, target, load_sem.at[i])
        for i, (source, target) in enumerate(
            (
                (decay_hbm, decay_ref),
                (dt_hbm, dt_ref),
                (b_hbm, b_ref),
                (c_hbm, c_ref),
                (skip_hbm, skip_ref),
            )
        )
    ]
    for copy in small:
        copy.start()

    chunk = 6144 // LOAD_CHUNKS
    loads_x, loads_dy = [], []
    for i in range(LOAD_CHUNKS):
        part = pl.ds(i * chunk, chunk)
        loads_x.append(pltpu.make_async_copy(x_hbm.at[0, :, part], xv.at[:, part], load_x_sem.at[i]))
        loads_dy.append(
            pltpu.make_async_copy(dy_hbm.at[0, :, part], dyv.at[:, part], load_dy_sem.at[i])
        )
    for i in range(LOAD_CHUNKS):
        loads_x[i].start()
        loads_dy[i].start()

    barrier = pltpu.get_barrier_semaphore()

    for dx in row_offsets:
        pl.semaphore_signal(barrier, inc=1, device_id=row_device(dx), device_id_type=MESH)
    for dz in column_offsets:
        pl.semaphore_signal(barrier, inc=1, device_id=column_device(dz), device_id_type=MESH)

    for copy in small:
        copy.wait()
    decay = decay_ref[0]
    dt = dt_ref[0]
    rows = lax.broadcasted_iota(jnp.int32, (SPAN, SPAN), 0)
    cols = lax.broadcasted_iota(jnp.int32, (SPAN, SPAN), 1)
    cum = plain_dot(decay, (rows <= cols).astype(jnp.float32), HIGHEST)
    from_start = jnp.exp(cum)
    to_end = dt * jnp.exp(cum[:, SPAN - 1 :] - cum)
    row_log = cum * LOG2E
    col_log = row_log - jnp.log(dt) * LOG2E
    for g in range(GROUPS):
        take = slice(g * HEADS_PER_GROUP, (g + 1) * HEADS_PER_GROUP)
        row_s[g, 0:HEADS_PER_GROUP, :] = row_log[take]
        col_s[g, 0:HEADS_PER_GROUP, :] = col_log[take]
        to_end_s[g, 0:HEADS_PER_GROUP, :] = to_end[take]
        from_start_s[g, 0:HEADS_PER_GROUP, :] = from_start[take]
    padded = jnp.concatenate([decay, jnp.zeros((32, SPAN), jnp.float32)], axis=0)
    total = nt_dot(jnp.ones((8, SPAN), jnp.float32), padded, HIGHEST)
    ends = jnp.exp(total[0:1])
    ends_high = ends.astype(jnp.bfloat16)
    rest = ends - ends_high.astype(jnp.float32)
    ends_mid = rest.astype(jnp.bfloat16)
    ends_low = rest - ends_mid.astype(jnp.float32)
    split_ends = jnp.concatenate(
        [
            ends_high.astype(jnp.float32),
            ends_mid.astype(jnp.float32),
            ends_low,
            jnp.zeros((13, HALF), jnp.float32),
        ],
        axis=0,
    ).astype(jnp.bfloat16)
    head_row = lax.broadcasted_iota(jnp.int32, (HALF, LANES), 0)
    lane_head = lax.broadcasted_iota(jnp.int32, (HALF, LANES), 1) // 64
    b_wide = b_ref[0].astype(jnp.float32)
    c_wide = c_ref[0].astype(jnp.float32)
    b_turned = jnp.transpose(b_wide).astype(jnp.bfloat16)
    cb_s[...] = plain_dot(b_turned, c_ref[0])
    mix_s[...] = jnp.zeros_like(mix_s)

    position = lax.broadcasted_iota(jnp.int32, (SPAN, 1), 0) + me * SPAN
    valid = (position < length_ref[0]).astype(jnp.float32).astype(jnp.bfloat16)
    low = lax.broadcasted_iota(jnp.int32, (STATE, HALF), 1) < 64

    def lanes_of(g):
        return pl.ds(pl.multiple_of(g * LANES, HALF), LANES)

    def per_head(wide, weights):
        return jnp.concatenate(
            [(wide * weights[k : k + 1, :]).astype(jnp.bfloat16) for k in range(HEADS_PER_GROUP)],
            axis=0,
        )

    def own_heads(product):
        pieces = []
        for k in range(3):
            block = product[32 * k : 32 * k + 32, HALF * k : HALF * k + HALF]
            pieces.append(jnp.where(low, block[:STATE], block[STATE:]))
        return jnp.concatenate(pieces, axis=1)

    def summary(g, carry):
        lanes = lanes_of(g)
        dy = dyv[:, lanes] * valid
        dyv[:, lanes] = dy
        state = own_heads(plain_dot(per_head(b_wide, to_end_s[g]), xv[:, lanes]))
        grad = own_heads(plain_dot(per_head(c_wide, from_start_s[g]), dy))
        for half in range(2):
            take = slice(8 * half, 8 * half + 8)
            both = jnp.concatenate([state[take], grad[take]], axis=0).astype(jnp.bfloat16)
            for c in range(CHUNKS):
                parts_out[c, g // 4, 2 * lax.rem(g, 4) + half] = both[:, HALF * c : HALF * c + HALF]
        pick = (head_row == lane_head + g * HEADS_PER_GROUP).astype(jnp.float32)
        wide = plain_dot(split_ends, pick.astype(jnp.bfloat16))
        ends_out[g // 4, :, pl.ds(pl.multiple_of(lax.rem(g, 4) * LANES, HALF), LANES)] = (
            wide[0:1] + wide[1:2] + wide[2:3]
        )
        return carry

    per_chunk = GROUPS // LOAD_CHUNKS
    for i in range(LOAD_CHUNKS):
        loads_x[i].wait()
        loads_dy[i].wait()
        lax.fori_loop(i * per_chunk, (i + 1) * per_chunk, summary, 0)

    pl.semaphore_wait(barrier, ROWS + COLUMNS - 2)

    def remote(source, target, slot, device):
        return pltpu.make_async_remote_copy(
            src_ref=source,
            dst_ref=target,
            send_sem=send_sem.at[slot],
            recv_sem=recv_sem.at[slot],
            device_id=device,
            device_id_type=MESH,
        )

    def row_wait(out_ref, in_ref, slot):
        few = pl.ds(0, ROWS - 1)
        return remote(out_ref.at[few], in_ref.at[few], slot, row_device(1))

    def column_wait(out_ref, in_ref, slot):
        few = pl.ds(0, COLUMNS - 1)
        return remote(out_ref.at[few], in_ref.at[few], slot, column_device(1))

    for dx in row_offsets:
        remote(ends_out.at[row_peer(dx)], ends_in.at[my_x], 12, row_device(dx)).start()
    def send_parts(c):
        for dx in row_offsets:
            remote(
                parts_out.at[c, row_peer(dx)], parts_in.at[c, my_x], c, row_device(dx)
            ).start()

    send_parts(0)
    for c in range(CHUNKS):
        parts_in[c, my_x] = parts_out[c, my_x]
    ends_in[my_x] = ends_out[my_x]

    causal = lax.broadcasted_iota(jnp.int32, (HALF, HALF), 0) <= lax.broadcasted_iota(
        jnp.int32, (HALF, HALF), 1
    )
    lane_row = lax.broadcasted_iota(jnp.int32, (1, HALF), 1)
    keep = (
        (lane_row < 64).astype(jnp.float32).astype(jnp.bfloat16),
        (lane_row >= 64).astype(jnp.float32).astype(jnp.bfloat16),
    )

    def within(g, carry):
        turned = jnp.transpose(col_s[g])
        logs = row_s[g]
        mix_aa = jnp.zeros((HALF, HALF), jnp.float32)
        mix_ab = jnp.zeros((HALF, HALF), jnp.float32)
        mix_bb = jnp.zeros((HALF, HALF), jnp.float32)
        for pair in range(3):
            lanes = pl.ds(pl.multiple_of(g * LANES + pair * HALF, HALF), HALF)
            x = xv[:, lanes]
            dy = dyv[:, lanes]
            first = jnp.zeros((HALF, HALF), jnp.float32)
            second = jnp.zeros((HALF, HALF), jnp.float32)
            for side in range(2):
                k = 2 * pair + side
                dy_one = dy * keep[side]
                score_a = nt_dot(x[:HALF], dy_one)
                score_b = nt_dot(x[HALF:], dy_one[HALF:])
                gap_aa = logs[k : k + 1, :HALF] - turned[:HALF, k : k + 1]
                gap_ab = logs[k : k + 1, HALF:] - turned[:HALF, k : k + 1]
                gap_bb = logs[k : k + 1, HALF:] - turned[HALF:, k : k + 1]
                fade_aa = jnp.exp2(jnp.where(causal, gap_aa, -jnp.inf))
                fade_ab = jnp.exp2(gap_ab)
                fade_bb = jnp.exp2(jnp.where(causal, gap_bb, -jnp.inf))
                mix_aa += fade_aa * score_a[:, :HALF]
                mix_ab += fade_ab * score_a[:, HALF:]
                mix_bb += fade_bb * score_b
                kernel_a = jnp.concatenate(
                    [
                        (fade_aa * cb_s[:HALF, :HALF]).astype(jnp.bfloat16),
                        (fade_ab * cb_s[:HALF, HALF:]).astype(jnp.bfloat16),
                    ],
                    axis=1,
                )
                kernel_b = (fade_bb * cb_s[HALF:, HALF:]).astype(jnp.bfloat16)
                first += plain_dot(kernel_a, dy_one)
                second += plain_dot(kernel_b, dy_one[HALF:])
            skip = jnp.where(
                lane_row < 64,
                skip_ref[HEADS_PER_GROUP * g + 2 * pair],
                skip_ref[HEADS_PER_GROUP * g + 2 * pair + 1],
            )
            direct = skip * dy.astype(jnp.float32)
            partial_x[:HALF, lanes] = first + direct[:HALF]
            partial_x[HALF:, lanes] = second + direct[HALF:]
        mix_s[:HALF, :HALF] += mix_aa
        mix_s[:HALF, HALF:] += mix_ab
        mix_s[HALF:, HALF:] += mix_bb
        return carry

    fills = list(FILL)
    done = [0]

    def fill():
        count = fills.pop(0)
        lax.fori_loop(done[0], done[0] + count, within, 0)
        done[0] += count

    def decay_rows(z, c):
        lanes = slice(LANES * (z // 2) + HALF * c, LANES * (z // 2) + HALF * c + HALF)
        return [ends_in[x, :, lanes] for x in range(ROWS)]

    def join_row(c):
        row_wait(parts_out.at[c], parts_in.at[c], c).wait_recv()
        if c == 0:
            row_wait(ends_out, ends_in, 12).wait_recv()
            quad = ends_in[0] * ends_in[1] * ends_in[2] * ends_in[3]
            for k in range(4):
                quad_out[k] = quad[:, LANES * k : LANES * k + LANES]
        for z in range(COLUMNS):
            decays = decay_rows(z, c)
            parts = [parts_in[c, x, z].astype(jnp.float32) for x in range(ROWS)]
            state = jnp.zeros((8, HALF), jnp.float32)
            states = []
            for x in range(ROWS):
                states.append(state)
                state = decays[x] * state + parts[x][:8]
            grad = jnp.zeros((8, HALF), jnp.float32)
            grads = [None] * ROWS
            for x in reversed(range(ROWS)):
                grads[x] = grad
                grad = decays[x] * grad + parts[x][8:]
            totals_out[c, z] = jnp.concatenate([state, grad], axis=0).astype(jnp.bfloat16)
            for x in range(ROWS):
                inside[c, x, z] = jnp.concatenate([states[x], grads[x]], axis=0)
        if c == 0:
            for dz in column_offsets:
                remote(
                    quad_out.at[column_peer(dz) // 2], quad_in.at[my_z], 13, column_device(dz)
                ).start()
            quad_in[my_z] = quad_out[my_z // 2]
        for dz in column_offsets:
            remote(
                totals_out.at[c, column_peer(dz)],
                totals_in.at[c, my_z],
                3 + c,
                column_device(dz),
            ).start()
        totals_in[c, my_z] = totals_out[c, my_z]

    def scan_column(c):
        column_wait(totals_out.at[c], totals_in.at[c], 3 + c).wait_recv()
        if c == 0:
            column_wait(quad_in, quad_in, 13).wait_recv()
        decays = [quad_in[z, :, HALF * c : HALF * c + HALF] for z in range(COLUMNS)]
        parts = [totals_in[c, z].astype(jnp.float32) for z in range(COLUMNS)]
        state = jnp.zeros((8, HALF), jnp.float32)
        states = []
        for z in range(COLUMNS):
            states.append(state)
            state = decays[z] * state + parts[z][:8]
        grad = jnp.zeros((8, HALF), jnp.float32)
        for z in reversed(range(COLUMNS)):
            before_out[c, z] = jnp.concatenate([states[z], grad], axis=0).astype(jnp.bfloat16)
            grad = decays[z] * grad + parts[z][8:]
        for dz in column_offsets:
            remote(
                before_out.at[c, column_peer(dz)],
                before_in.at[c, my_z],
                6 + c,
                column_device(dz),
            ).start()
        before_in[c, my_z] = before_out[c, my_z]

    def finish_row(c):
        column_wait(before_out.at[c], before_in.at[c], 6 + c).wait_recv()
        for z in range(COLUMNS):
            decays = decay_rows(z, c)
            outside = before_in[c, z].astype(jnp.float32)
            state = outside[:8]
            states = []
            for x in range(ROWS):
                states.append(state)
                if x < ROWS - 1:
                    state = decays[x] * state
            grad = outside[8:]
            for x in reversed(range(ROWS)):
                entering = jnp.concatenate([states[x], grad], axis=0) + inside[c, x, z]
                states_out[c, x, z] = entering.astype(jnp.bfloat16)
                if x > 0:
                    grad = decays[x] * grad
        for dx in row_offsets:
            remote(
                states_out.at[c, row_peer(dx)], states_in.at[c, my_x], 9 + c, row_device(dx)
            ).start()
        states_in[c, my_x] = states_out[c, my_x]

    for c in range(1, CHUNKS):
        fill()
        send_parts(c)
    for stage in (join_row, scan_column, finish_row):
        for c in range(CHUNKS):
            fill()
            stage(c)
    fill()

    def turned_rows(c, g):
        first = states_in[c, g // 4, 2 * lax.rem(g, 4)].astype(jnp.float32)
        second = states_in[c, g // 4, 2 * lax.rem(g, 4) + 1].astype(jnp.float32)
        return (
            jnp.concatenate([first[:8], second[:8]], axis=0).astype(jnp.bfloat16),
            jnp.concatenate([first[8:], second[8:]], axis=0).astype(jnp.bfloat16),
        )

    def spread(one, two):
        blank = jnp.zeros((2 * STATE, HALF), jnp.bfloat16)
        top = jnp.concatenate([one * keep[0], one * keep[1]], axis=0)
        bottom = jnp.concatenate([two * keep[0], two * keep[1]], axis=0)
        return jnp.concatenate(
            [
                jnp.concatenate([top, blank], axis=1),
                jnp.concatenate([blank, bottom], axis=1),
            ],
            axis=0,
        )

    def across(c, pair, carry):
        cross_b, cross_c = carry
        groups = (2 * pair, 2 * pair + 1)
        lanes = [pl.ds(pl.multiple_of(g * LANES + HALF * c, HALF), HALF) for g in groups]
        state_one, grad_one = turned_rows(c, groups[0])
        state_two, grad_two = turned_rows(c, groups[1])
        state = spread(state_one, state_two)
        grad = spread(grad_one, grad_two)
        heads = slice(2 * c, 2 * c + 2)
        ends = jnp.concatenate([to_end_s[g][heads] for g in groups], axis=0)
        starts = jnp.concatenate([from_start_s[g][heads] for g in groups], axis=0)
        into = jnp.concatenate([b_wide * ends[k : k + 1, :] for k in range(4)], axis=0)
        term = plain_dot(jnp.transpose(into).astype(jnp.bfloat16), grad)
        for k in range(2):
            gx_ref[0, :, lanes[k]] = (
                partial_x[:, lanes[k]] + term[:, HALF * k : HALF * k + HALF]
            ).astype(jnp.bfloat16)
        x = jnp.concatenate([xv[:, part] for part in lanes], axis=1)
        dy = jnp.concatenate([dyv[:, part] for part in lanes], axis=1)
        from_x = nt_dot(grad, x)
        from_dy = nt_dot(state, dy)
        for k in range(4):
            take = slice(STATE * k, STATE * k + STATE)
            cross_b += from_x[take] * ends[k : k + 1, :]
            cross_c += from_dy[take] * starts[k : k + 1, :]
        return cross_b, cross_c

    zero = jnp.zeros((STATE, SPAN), jnp.float32)
    crosses = (zero, zero)
    for c in range(CHUNKS):
        row_wait(states_out.at[c], states_in.at[c], 9 + c).wait_recv()
        crosses = lax.fori_loop(
            0,
            GROUPS // 4,
            lambda two, carry, c=c: across(c, 2 * two + 1, across(c, 2 * two, carry)),
            crosses,
        )
    cross_b, cross_c = crosses
    mixing = mix_s[...]
    gb_ref[0] = (nt_dot(c_wide, mixing, HIGHEST) + cross_b) * scale_b
    gc_ref[0] = (plain_dot(b_wide, mixing, HIGHEST) + cross_c) * scale_c

    for c in range(CHUNKS):
        row_wait(parts_out.at[c], parts_in.at[c], c).wait_send()
        column_wait(totals_out.at[c], totals_in.at[c], 3 + c).wait_send()
        column_wait(before_out.at[c], before_in.at[c], 6 + c).wait_send()
        row_wait(states_out.at[c], states_in.at[c], 9 + c).wait_send()
    row_wait(ends_out, ends_in, 12).wait_send()
    column_wait(quad_in, quad_in, 13).wait_send()


def store_results(gx_ref, gb_ref, gc_ref, gx_hbm, gb_hbm, gc_hbm, sem):
    copies = []
    for i in range(8):
        part = pl.ds(32 * i, 32)
        copies.append(
            pltpu.make_async_copy(gx_ref.at[0, part], gx_hbm.at[0, part], sem.at[i])
        )
    copies.append(pltpu.make_async_copy(gb_ref, gb_hbm, sem.at[8]))
    copies.append(pltpu.make_async_copy(gc_ref, gc_hbm, sem.at[9]))
    for copy in copies:
        copy.start()
    for copy in copies:
        copy.wait()


def solution(mesh):
    def local(inputs, out_grad, step_size, log_decay, b_matrix, c_matrix, skip_gain, lengths):
        columns = inputs.shape[2]
        scale_b = 1.0 / math.sqrt(columns)
        scale_c = math.sqrt(STATE / (columns * PEERS * SPAN))
        vmem = pl.BlockSpec(memory_space=pltpu.VMEM)
        whole = pl.BlockSpec(memory_space=pltpu.HBM)
        f32, bf16 = jnp.float32, jnp.bfloat16
        shapes = (
            jax.ShapeDtypeStruct(inputs.shape, bf16),
            jax.ShapeDtypeStruct(b_matrix.shape, f32),
            jax.ShapeDtypeStruct(c_matrix.shape, f32),
        )
        results = pl.pallas_call(
            lambda *refs: kernel(scale_b, scale_c, *refs),
            out_shape=tuple(pltpu.VMEM(shape.shape, shape.dtype) for shape in shapes),
            in_specs=[pl.BlockSpec(memory_space=pltpu.SMEM)] + [whole] * 7,
            out_specs=(vmem, vmem, vmem),
            scratch_shapes=[
                pltpu.SMEM((96,), f32),
                pltpu.VMEM((1, 96, SPAN), f32),
                pltpu.VMEM((1, 96, SPAN), f32),
                pltpu.VMEM((1, STATE, SPAN), bf16),
                pltpu.VMEM((1, STATE, SPAN), bf16),
                pltpu.VMEM((SPAN, columns), bf16),
                pltpu.VMEM((SPAN, columns), bf16),
                pltpu.VMEM((SPAN, columns), f32),
                pltpu.VMEM((GROUPS, 8, SPAN), f32),
                pltpu.VMEM((GROUPS, 8, SPAN), f32),
                pltpu.VMEM((GROUPS, 8, SPAN), f32),
                pltpu.VMEM((GROUPS, 8, SPAN), f32),
                pltpu.VMEM((SPAN, SPAN), f32),
                pltpu.VMEM((SPAN, SPAN), f32),
                pltpu.VMEM((CHUNKS, ROWS, COLUMNS, 16, HALF), bf16),
                pltpu.VMEM((CHUNKS, ROWS, COLUMNS, 16, HALF), bf16),
                pltpu.VMEM((ROWS, 1, QUARTER), f32),
                pltpu.VMEM((ROWS, 1, QUARTER), f32),
                pltpu.VMEM((CHUNKS, ROWS, COLUMNS, 16, HALF), f32),
                pltpu.VMEM((CHUNKS, COLUMNS, 16, HALF), bf16),
                pltpu.VMEM((CHUNKS, COLUMNS, 16, HALF), bf16),
                pltpu.VMEM((4, 1, LANES), f32),
                pltpu.VMEM((COLUMNS, 1, LANES), f32),
                pltpu.VMEM((CHUNKS, COLUMNS, 16, HALF), bf16),
                pltpu.VMEM((CHUNKS, COLUMNS, 16, HALF), bf16),
                pltpu.VMEM((CHUNKS, ROWS, COLUMNS, 16, HALF), bf16),
                pltpu.VMEM((CHUNKS, ROWS, COLUMNS, 16, HALF), bf16),
                pltpu.SemaphoreType.DMA((LOAD_CHUNKS,)),
                pltpu.SemaphoreType.DMA((LOAD_CHUNKS,)),
                pltpu.SemaphoreType.DMA((5,)),
                pltpu.SemaphoreType.DMA((14,)),
                pltpu.SemaphoreType.DMA((14,)),
            ],
            compiler_params=pltpu.CompilerParams(
                collective_id=0, has_side_effects=True, vmem_limit_bytes=48 * 1024 * 1024
            ),
        )(
            lengths,
            *(
                pltpu.with_memory_space_constraint(operand, pltpu.HBM)
                for operand in (
                    skip_gain,
                    inputs,
                    out_grad,
                    step_size,
                    log_decay,
                    b_matrix,
                    c_matrix,
                )
            )
        )
        return pl.pallas_call(
            store_results,
            out_shape=shapes,
            in_specs=[vmem] * 3,
            out_specs=(whole,) * 3,
            scratch_shapes=[pltpu.SemaphoreType.DMA((10,))],
        )(*(pltpu.with_memory_space_constraint(result, pltpu.VMEM) for result in results))

    return jax.shard_map(
        local,
        mesh=mesh,
        in_specs=(
            P("batch", "seq", None),
            P("batch", "seq", None),
            P("batch", None, "seq"),
            P("batch", None, "seq"),
            P("batch", None, "seq"),
            P("batch", None, "seq"),
            P(),
            P("batch"),
        ),
        out_specs=(P("batch", "seq", None), P("batch", None, "seq"), P("batch", None, "seq")),
        check_vma=False,
    )
```

```python
import math

import jax
import jax.numpy as jnp
from jax import lax
from jax.experimental import pallas as pl
from jax.experimental.pallas import tpu as pltpu
from jax.sharding import PartitionSpec as P

MESH = pl.DeviceIdType.MESH
HIGHEST = lax.Precision.HIGHEST
LOG2E = 1.4426950408889634
SPAN = 256
HALF = 128
STATE = 16
HEADS_PER_GROUP = 6
LANES = 384
GROUPS = 16
PEERS = 32
LOAD_CHUNKS = 4
ROWS = 4
COLUMNS = 8
CHUNKS = 3
QUARTER = 1536
FILL = (2, 1, 1, 2, 1, 2, 2, 1, 1, 2, 1)
NT = (((1,), (1,)), ((), ()))


def nt_dot(a, b, precision=None):
    return lax.dot_general(a, b, NT, precision=precision, preferred_element_type=jnp.float32)


def plain_dot(a, b, precision=None):
    return jnp.dot(a, b, precision=precision, preferred_element_type=jnp.float32)


def kernel(
    scale_b,
    scale_c,
    length_ref,
    skip_hbm,
    x_hbm,
    dy_hbm,
    dt_hbm,
    decay_hbm,
    b_hbm,
    c_hbm,
    gx_ref,
    gb_ref,
    gc_ref,
    skip_ref,
    dt_ref,
    decay_ref,
    b_ref,
    c_ref,
    xv,
    dyv,
    partial_x,
    row_s,
    col_s,
    to_end_s,
    from_start_s,
    cb_s,
    mix_s,
    parts_out,
    parts_in,
    ends_out,
    ends_in,
    inside,
    totals_out,
    totals_in,
    quad_out,
    quad_in,
    before_out,
    before_in,
    states_out,
    states_in,
    load_x_sem,
    load_dy_sem,
    load_sem,
    send_sem,
    recv_sem,
):
    me = lax.axis_index("seq")
    lane_of_batch = lax.axis_index("batch")

    my_z = me // ROWS
    my_x = lax.rem(me, ROWS)
    row_offsets = (2, 1, 3)
    column_offsets = (4, 3, 5, 2, 6, 1, 7)

    def row_peer(dx):
        return lax.rem(my_x + dx, ROWS)

    def column_peer(dz):
        return lax.rem(my_z + dz, COLUMNS)

    def row_device(dx):
        return (my_z * ROWS + row_peer(dx), lane_of_batch)

    def column_device(dz):
        return (column_peer(dz) * ROWS + my_x, lane_of_batch)

    small = [
        pltpu.make_async_copy(source, target, load_sem.at[i])
        for i, (source, target) in enumerate(
            (
                (decay_hbm, decay_ref),
                (dt_hbm, dt_ref),
                (b_hbm, b_ref),
                (c_hbm, c_ref),
                (skip_hbm, skip_ref),
            )
        )
    ]
    for copy in small:
        copy.start()

    quarters = [row_peer(dx) for dx in row_offsets + (0,)]
    loads_x, loads_dy = [], []
    for i, quarter in enumerate(quarters):
        part = pl.ds(pl.multiple_of(quarter * QUARTER, HALF), QUARTER)
        loads_x.append(pltpu.make_async_copy(x_hbm.at[0, :, part], xv.at[:, part], load_x_sem.at[i]))
        loads_dy.append(
            pltpu.make_async_copy(dy_hbm.at[0, :, part], dyv.at[:, part], load_dy_sem.at[i])
        )
    for i in range(LOAD_CHUNKS):
        loads_x[i].start()
        loads_dy[i].start()

    barrier = pltpu.get_barrier_semaphore()

    for dx in row_offsets:
        pl.semaphore_signal(barrier, inc=1, device_id=row_device(dx), device_id_type=MESH)
    for dz in column_offsets:
        pl.semaphore_signal(barrier, inc=1, device_id=column_device(dz), device_id_type=MESH)

    for copy in small:
        copy.wait()
    decay = decay_ref[0]
    dt = dt_ref[0]
    rows = lax.broadcasted_iota(jnp.int32, (SPAN, SPAN), 0)
    cols = lax.broadcasted_iota(jnp.int32, (SPAN, SPAN), 1)
    cum = plain_dot(decay, (rows <= cols).astype(jnp.float32), HIGHEST)
    from_start = jnp.exp(cum)
    to_end = dt * jnp.exp(cum[:, SPAN - 1 :] - cum)
    row_log = cum * LOG2E
    col_log = row_log - jnp.log(dt) * LOG2E
    for g in range(GROUPS):
        take = slice(g * HEADS_PER_GROUP, (g + 1) * HEADS_PER_GROUP)
        row_s[g, 0:HEADS_PER_GROUP, :] = row_log[take]
        col_s[g, 0:HEADS_PER_GROUP, :] = col_log[take]
        to_end_s[g, 0:HEADS_PER_GROUP, :] = to_end[take]
        from_start_s[g, 0:HEADS_PER_GROUP, :] = from_start[take]
    padded = jnp.concatenate([decay, jnp.zeros((32, SPAN), jnp.float32)], axis=0)
    total = nt_dot(jnp.ones((8, SPAN), jnp.float32), padded, HIGHEST)
    ends = jnp.exp(total[0:1])
    ends_high = ends.astype(jnp.bfloat16)
    rest = ends - ends_high.astype(jnp.float32)
    ends_mid = rest.astype(jnp.bfloat16)
    ends_low = rest - ends_mid.astype(jnp.float32)
    split_ends = jnp.concatenate(
        [
            ends_high.astype(jnp.float32),
            ends_mid.astype(jnp.float32),
            ends_low,
            jnp.zeros((13, HALF), jnp.float32),
        ],
        axis=0,
    ).astype(jnp.bfloat16)
    head_row = lax.broadcasted_iota(jnp.int32, (HALF, LANES), 0)
    lane_head = lax.broadcasted_iota(jnp.int32, (HALF, LANES), 1) // 64
    b_wide = b_ref[0].astype(jnp.float32)
    c_wide = c_ref[0].astype(jnp.float32)
    b_turned = jnp.transpose(b_wide).astype(jnp.bfloat16)
    cb_s[...] = plain_dot(b_turned, c_ref[0])
    mix_s[...] = jnp.zeros_like(mix_s)

    position = lax.broadcasted_iota(jnp.int32, (SPAN, 1), 0) + me * SPAN
    valid = (position < length_ref[0]).astype(jnp.float32).astype(jnp.bfloat16)
    low = lax.broadcasted_iota(jnp.int32, (STATE, HALF), 1) < 64

    def lanes_of(g):
        return pl.ds(pl.multiple_of(g * LANES, HALF), LANES)

    def per_head(wide, weights):
        return jnp.concatenate(
            [(wide * weights[k : k + 1, :]).astype(jnp.bfloat16) for k in range(HEADS_PER_GROUP)],
            axis=0,
        )

    def own_heads(product):
        pieces = []
        for k in range(3):
            block = product[32 * k : 32 * k + 32, HALF * k : HALF * k + HALF]
            pieces.append(jnp.where(low, block[:STATE], block[STATE:]))
        return jnp.concatenate(pieces, axis=1)

    def summary(g, carry):
        lanes = lanes_of(g)
        dy = dyv[:, lanes] * valid
        dyv[:, lanes] = dy
        state = own_heads(plain_dot(per_head(b_wide, to_end_s[g]), xv[:, lanes]))
        grad = own_heads(plain_dot(per_head(c_wide, from_start_s[g]), dy))
        for half in range(2):
            take = slice(8 * half, 8 * half + 8)
            both = jnp.concatenate([state[take], grad[take]], axis=0).astype(jnp.bfloat16)
            for c in range(CHUNKS):
                parts_out[c, g // 4, 2 * lax.rem(g, 4) + half] = both[:, HALF * c : HALF * c + HALF]
        pick = (head_row == lane_head + g * HEADS_PER_GROUP).astype(jnp.float32)
        wide = plain_dot(split_ends, pick.astype(jnp.bfloat16))
        ends_out[g // 4, :, pl.ds(pl.multiple_of(lax.rem(g, 4) * LANES, HALF), LANES)] = (
            wide[0:1] + wide[1:2] + wide[2:3]
        )
        return carry

    def remote(source, target, slot, device):
        return pltpu.make_async_remote_copy(
            src_ref=source,
            dst_ref=target,
            send_sem=send_sem.at[slot],
            recv_sem=recv_sem.at[slot],
            device_id=device,
            device_id_type=MESH,
        )

    def row_wait(out_ref, in_ref, slot):
        few = pl.ds(0, ROWS - 1)
        return remote(out_ref.at[few], in_ref.at[few], slot, row_device(1))

    def column_wait(out_ref, in_ref, slot):
        few = pl.ds(0, COLUMNS - 1)
        return remote(out_ref.at[few], in_ref.at[few], slot, column_device(1))

    def send_part(c, dx):
        remote(
            parts_out.at[c, row_peer(dx)], parts_in.at[c, my_x], c, row_device(dx)
        ).start()

    def send_parts(c):
        for dx in row_offsets:
            send_part(c, dx)

    for i, quarter in enumerate(quarters):
        loads_x[i].wait()
        loads_dy[i].wait()
        lax.fori_loop(
            0,
            2,
            lambda k, carry, first=4 * quarter: summary(
                first + 2 * k + 1, summary(first + 2 * k, carry)
            ),
            0,
        )
        if i == 0:
            pl.semaphore_wait(barrier, ROWS + COLUMNS - 2)
        if i < ROWS - 1:
            dx = row_offsets[i]
            remote(ends_out.at[quarter], ends_in.at[my_x], 12, row_device(dx)).start()
            send_part(0, dx)
    send_parts(1)
    for c in range(CHUNKS):
        parts_in[c, my_x] = parts_out[c, my_x]
    ends_in[my_x] = ends_out[my_x]

    causal = lax.broadcasted_iota(jnp.int32, (HALF, HALF), 0) <= lax.broadcasted_iota(
        jnp.int32, (HALF, HALF), 1
    )
    lane_row = lax.broadcasted_iota(jnp.int32, (1, HALF), 1)
    keep = (
        (lane_row < 64).astype(jnp.float32).astype(jnp.bfloat16),
        (lane_row >= 64).astype(jnp.float32).astype(jnp.bfloat16),
    )

    def within(g, carry):
        turned = jnp.transpose(col_s[g])
        logs = row_s[g]
        mix_aa = jnp.zeros((HALF, HALF), jnp.float32)
        mix_ab = jnp.zeros((HALF, HALF), jnp.float32)
        mix_bb = jnp.zeros((HALF, HALF), jnp.float32)
        for pair in range(3):
            lanes = pl.ds(pl.multiple_of(g * LANES + pair * HALF, HALF), HALF)
            x = xv[:, lanes]
            dy = dyv[:, lanes]
            first = jnp.zeros((HALF, HALF), jnp.float32)
            second = jnp.zeros((HALF, HALF), jnp.float32)
            for side in range(2):
                k = 2 * pair + side
                dy_one = dy * keep[side]
                score_a = nt_dot(x[:HALF], dy_one)
                score_b = nt_dot(x[HALF:], dy_one[HALF:])
                gap_aa = logs[k : k + 1, :HALF] - turned[:HALF, k : k + 1]
                gap_ab = logs[k : k + 1, HALF:] - turned[:HALF, k : k + 1]
                gap_bb = logs[k : k + 1, HALF:] - turned[HALF:, k : k + 1]
                fade_aa = jnp.exp2(jnp.where(causal, gap_aa, -jnp.inf))
                fade_ab = jnp.exp2(gap_ab)
                fade_bb = jnp.exp2(jnp.where(causal, gap_bb, -jnp.inf))
                mix_aa += fade_aa * score_a[:, :HALF]
                mix_ab += fade_ab * score_a[:, HALF:]
                mix_bb += fade_bb * score_b
                kernel_a = jnp.concatenate(
                    [
                        (fade_aa * cb_s[:HALF, :HALF]).astype(jnp.bfloat16),
                        (fade_ab * cb_s[:HALF, HALF:]).astype(jnp.bfloat16),
                    ],
                    axis=1,
                )
                kernel_b = (fade_bb * cb_s[HALF:, HALF:]).astype(jnp.bfloat16)
                first += plain_dot(kernel_a, dy_one)
                second += plain_dot(kernel_b, dy_one[HALF:])
            skip = jnp.where(
                lane_row < 64,
                skip_ref[HEADS_PER_GROUP * g + 2 * pair],
                skip_ref[HEADS_PER_GROUP * g + 2 * pair + 1],
            )
            direct = skip * dy.astype(jnp.float32)
            partial_x[:HALF, lanes] = first + direct[:HALF]
            partial_x[HALF:, lanes] = second + direct[HALF:]
        mix_s[:HALF, :HALF] += mix_aa
        mix_s[:HALF, HALF:] += mix_ab
        mix_s[HALF:, HALF:] += mix_bb
        return carry

    fills = list(FILL)
    done = [0]

    def fill():
        count = fills.pop(0)
        lax.fori_loop(done[0], done[0] + count, within, 0)
        done[0] += count

    def decay_rows(z, c):
        lanes = slice(LANES * (z // 2) + HALF * c, LANES * (z // 2) + HALF * c + HALF)
        return [ends_in[x, :, lanes] for x in range(ROWS)]

    def join_row(c):
        row_wait(parts_out.at[c], parts_in.at[c], c).wait_recv()
        if c == 0:
            row_wait(ends_out, ends_in, 12).wait_recv()
            quad = ends_in[0] * ends_in[1] * ends_in[2] * ends_in[3]
            for k in range(4):
                quad_out[k] = quad[:, LANES * k : LANES * k + LANES]
        for z in range(COLUMNS):
            decays = decay_rows(z, c)
            parts = [parts_in[c, x, z].astype(jnp.float32) for x in range(ROWS)]
            state = jnp.zeros((8, HALF), jnp.float32)
            states = []
            for x in range(ROWS):
                states.append(state)
                state = decays[x] * state + parts[x][:8]
            grad = jnp.zeros((8, HALF), jnp.float32)
            grads = [None] * ROWS
            for x in reversed(range(ROWS)):
                grads[x] = grad
                grad = decays[x] * grad + parts[x][8:]
            totals_out[c, z] = jnp.concatenate([state, grad], axis=0).astype(jnp.bfloat16)
            for x in range(ROWS):
                inside[c, x, z] = jnp.concatenate([states[x], grads[x]], axis=0)
        if c == 0:
            for dz in column_offsets:
                remote(
                    quad_out.at[column_peer(dz) // 2], quad_in.at[my_z], 13, column_device(dz)
                ).start()
            quad_in[my_z] = quad_out[my_z // 2]
        for dz in column_offsets:
            remote(
                totals_out.at[c, column_peer(dz)],
                totals_in.at[c, my_z],
                3 + c,
                column_device(dz),
            ).start()
        totals_in[c, my_z] = totals_out[c, my_z]

    def scan_column(c):
        column_wait(totals_out.at[c], totals_in.at[c], 3 + c).wait_recv()
        if c == 0:
            column_wait(quad_in, quad_in, 13).wait_recv()
        decays = [quad_in[z, :, HALF * c : HALF * c + HALF] for z in range(COLUMNS)]
        parts = [totals_in[c, z].astype(jnp.float32) for z in range(COLUMNS)]
        state = jnp.zeros((8, HALF), jnp.float32)
        states = []
        for z in range(COLUMNS):
            states.append(state)
            state = decays[z] * state + parts[z][:8]
        grad = jnp.zeros((8, HALF), jnp.float32)
        for z in reversed(range(COLUMNS)):
            before_out[c, z] = jnp.concatenate([states[z], grad], axis=0).astype(jnp.bfloat16)
            grad = decays[z] * grad + parts[z][8:]
        for dz in column_offsets:
            remote(
                before_out.at[c, column_peer(dz)],
                before_in.at[c, my_z],
                6 + c,
                column_device(dz),
            ).start()
        before_in[c, my_z] = before_out[c, my_z]

    def finish_row(c):
        column_wait(before_out.at[c], before_in.at[c], 6 + c).wait_recv()
        for z in range(COLUMNS):
            decays = decay_rows(z, c)
            outside = before_in[c, z].astype(jnp.float32)
            state = outside[:8]
            states = []
            for x in range(ROWS):
                states.append(state)
                if x < ROWS - 1:
                    state = decays[x] * state
            grad = outside[8:]
            for x in reversed(range(ROWS)):
                entering = jnp.concatenate([states[x], grad], axis=0) + inside[c, x, z]
                states_out[c, x, z] = entering.astype(jnp.bfloat16)
                if x > 0:
                    grad = decays[x] * grad
        for dx in row_offsets:
            remote(
                states_out.at[c, row_peer(dx)], states_in.at[c, my_x], 9 + c, row_device(dx)
            ).start()
        states_in[c, my_x] = states_out[c, my_x]

    fill()
    send_parts(2)
    for stage in (join_row, scan_column, finish_row):
        for c in range(CHUNKS):
            fill()
            stage(c)
    fill()
    mixing = mix_s[...]
    base_b = nt_dot(c_wide, mixing, HIGHEST)
    base_c = plain_dot(b_wide, mixing, HIGHEST)

    def turned_rows(c, g):
        first = states_in[c, g // 4, 2 * lax.rem(g, 4)].astype(jnp.float32)
        second = states_in[c, g // 4, 2 * lax.rem(g, 4) + 1].astype(jnp.float32)
        return (
            jnp.concatenate([first[:8], second[:8]], axis=0).astype(jnp.bfloat16),
            jnp.concatenate([first[8:], second[8:]], axis=0).astype(jnp.bfloat16),
        )

    def spread(one, two):
        blank = jnp.zeros((2 * STATE, HALF), jnp.bfloat16)
        top = jnp.concatenate([one * keep[0], one * keep[1]], axis=0)
        bottom = jnp.concatenate([two * keep[0], two * keep[1]], axis=0)
        return jnp.concatenate(
            [
                jnp.concatenate([top, blank], axis=1),
                jnp.concatenate([blank, bottom], axis=1),
            ],
            axis=0,
        )

    def across(c, pair, carry):
        cross_b, cross_c = carry
        groups = (2 * pair, 2 * pair + 1)
        lanes = [pl.ds(pl.multiple_of(g * LANES + HALF * c, HALF), HALF) for g in groups]
        state_one, grad_one = turned_rows(c, groups[0])
        state_two, grad_two = turned_rows(c, groups[1])
        state = spread(state_one, state_two)
        grad = spread(grad_one, grad_two)
        heads = slice(2 * c, 2 * c + 2)
        ends = jnp.concatenate([to_end_s[g][heads] for g in groups], axis=0)
        starts = jnp.concatenate([from_start_s[g][heads] for g in groups], axis=0)
        into = jnp.concatenate([b_wide * ends[k : k + 1, :] for k in range(4)], axis=0)
        term = plain_dot(jnp.transpose(into).astype(jnp.bfloat16), grad)
        for k in range(2):
            gx_ref[0, :, lanes[k]] = (
                partial_x[:, lanes[k]] + term[:, HALF * k : HALF * k + HALF]
            ).astype(jnp.bfloat16)
        x = jnp.concatenate([xv[:, part] for part in lanes], axis=1)
        dy = jnp.concatenate([dyv[:, part] for part in lanes], axis=1)
        from_x = nt_dot(grad, x)
        from_dy = nt_dot(state, dy)
        for k in range(4):
            take = slice(STATE * k, STATE * k + STATE)
            cross_b += from_x[take] * ends[k : k + 1, :]
            cross_c += from_dy[take] * starts[k : k + 1, :]
        return cross_b, cross_c

    crosses = (base_b, base_c)
    for c in range(CHUNKS):
        row_wait(states_out.at[c], states_in.at[c], 9 + c).wait_recv()
        crosses = lax.fori_loop(
            0,
            GROUPS // 4,
            lambda two, carry, c=c: across(c, 2 * two + 1, across(c, 2 * two, carry)),
            crosses,
        )
    cross_b, cross_c = crosses
    gb_ref[0] = cross_b * scale_b
    gc_ref[0] = cross_c * scale_c

    for c in range(CHUNKS):
        row_wait(parts_out.at[c], parts_in.at[c], c).wait_send()
        column_wait(totals_out.at[c], totals_in.at[c], 3 + c).wait_send()
        column_wait(before_out.at[c], before_in.at[c], 6 + c).wait_send()
        row_wait(states_out.at[c], states_in.at[c], 9 + c).wait_send()
    row_wait(ends_out, ends_in, 12).wait_send()
    column_wait(quad_in, quad_in, 13).wait_send()


def store_results(gx_ref, gb_ref, gc_ref, gx_hbm, gb_hbm, gc_hbm, sem):
    copies = []
    for i in range(8):
        part = pl.ds(32 * i, 32)
        copies.append(
            pltpu.make_async_copy(gx_ref.at[0, part], gx_hbm.at[0, part], sem.at[i])
        )
    copies.append(pltpu.make_async_copy(gb_ref, gb_hbm, sem.at[8]))
    copies.append(pltpu.make_async_copy(gc_ref, gc_hbm, sem.at[9]))
    for copy in copies:
        copy.start()
    for copy in copies:
        copy.wait()


def solution(mesh):
    def local(inputs, out_grad, step_size, log_decay, b_matrix, c_matrix, skip_gain, lengths):
        columns = inputs.shape[2]
        scale_b = 1.0 / math.sqrt(columns)
        scale_c = math.sqrt(STATE / (columns * PEERS * SPAN))
        vmem = pl.BlockSpec(memory_space=pltpu.VMEM)
        whole = pl.BlockSpec(memory_space=pltpu.HBM)
        f32, bf16 = jnp.float32, jnp.bfloat16
        shapes = (
            jax.ShapeDtypeStruct(inputs.shape, bf16),
            jax.ShapeDtypeStruct(b_matrix.shape, f32),
            jax.ShapeDtypeStruct(c_matrix.shape, f32),
        )
        results = pl.pallas_call(
            lambda *refs: kernel(scale_b, scale_c, *refs),
            out_shape=tuple(pltpu.VMEM(shape.shape, shape.dtype) for shape in shapes),
            in_specs=[pl.BlockSpec(memory_space=pltpu.SMEM)] + [whole] * 7,
            out_specs=(vmem, vmem, vmem),
            scratch_shapes=[
                pltpu.SMEM((96,), f32),
                pltpu.VMEM((1, 96, SPAN), f32),
                pltpu.VMEM((1, 96, SPAN), f32),
                pltpu.VMEM((1, STATE, SPAN), bf16),
                pltpu.VMEM((1, STATE, SPAN), bf16),
                pltpu.VMEM((SPAN, columns), bf16),
                pltpu.VMEM((SPAN, columns), bf16),
                pltpu.VMEM((SPAN, columns), f32),
                pltpu.VMEM((GROUPS, 8, SPAN), f32),
                pltpu.VMEM((GROUPS, 8, SPAN), f32),
                pltpu.VMEM((GROUPS, 8, SPAN), f32),
                pltpu.VMEM((GROUPS, 8, SPAN), f32),
                pltpu.VMEM((SPAN, SPAN), f32),
                pltpu.VMEM((SPAN, SPAN), f32),
                pltpu.VMEM((CHUNKS, ROWS, COLUMNS, 16, HALF), bf16),
                pltpu.VMEM((CHUNKS, ROWS, COLUMNS, 16, HALF), bf16),
                pltpu.VMEM((ROWS, 1, QUARTER), f32),
                pltpu.VMEM((ROWS, 1, QUARTER), f32),
                pltpu.VMEM((CHUNKS, ROWS, COLUMNS, 16, HALF), f32),
                pltpu.VMEM((CHUNKS, COLUMNS, 16, HALF), bf16),
                pltpu.VMEM((CHUNKS, COLUMNS, 16, HALF), bf16),
                pltpu.VMEM((4, 1, LANES), f32),
                pltpu.VMEM((COLUMNS, 1, LANES), f32),
                pltpu.VMEM((CHUNKS, COLUMNS, 16, HALF), bf16),
                pltpu.VMEM((CHUNKS, COLUMNS, 16, HALF), bf16),
                pltpu.VMEM((CHUNKS, ROWS, COLUMNS, 16, HALF), bf16),
                pltpu.VMEM((CHUNKS, ROWS, COLUMNS, 16, HALF), bf16),
                pltpu.SemaphoreType.DMA((LOAD_CHUNKS,)),
                pltpu.SemaphoreType.DMA((LOAD_CHUNKS,)),
                pltpu.SemaphoreType.DMA((5,)),
                pltpu.SemaphoreType.DMA((14,)),
                pltpu.SemaphoreType.DMA((14,)),
            ],
            compiler_params=pltpu.CompilerParams(
                collective_id=0, has_side_effects=True, vmem_limit_bytes=48 * 1024 * 1024
            ),
        )(
            lengths,
            *(
                pltpu.with_memory_space_constraint(operand, pltpu.HBM)
                for operand in (
                    skip_gain,
                    inputs,
                    out_grad,
                    step_size,
                    log_decay,
                    b_matrix,
                    c_matrix,
                )
            )
        )
        return pl.pallas_call(
            store_results,
            out_shape=shapes,
            in_specs=[vmem] * 3,
            out_specs=(whole,) * 3,
            scratch_shapes=[pltpu.SemaphoreType.DMA((10,))],
        )(*(pltpu.with_memory_space_constraint(result, pltpu.VMEM) for result in results))

    return jax.shard_map(
        local,
        mesh=mesh,
        in_specs=(
            P("batch", "seq", None),
            P("batch", "seq", None),
            P("batch", None, "seq"),
            P("batch", None, "seq"),
            P("batch", None, "seq"),
            P("batch", None, "seq"),
            P(),
            P("batch"),
        ),
        out_specs=(P("batch", "seq", None), P("batch", None, "seq"), P("batch", None, "seq")),
        check_vma=False,
    )
```

```python
import math

import jax
import jax.numpy as jnp
from jax import lax
from jax.experimental import pallas as pl
from jax.experimental.pallas import tpu as pltpu
from jax.sharding import PartitionSpec as P

MESH = pl.DeviceIdType.MESH
HIGHEST = lax.Precision.HIGHEST
LOG2E = 1.4426950408889634
SPAN = 256
HALF = 128
STATE = 16
HEADS_PER_GROUP = 6
LANES = 384
GROUPS = 16
PEERS = 32
LOAD_CHUNKS = 4
ROWS = 4
COLUMNS = 8
CHUNKS = 3
QUARTER = 1536
FILL = (2, 1, 1, 2, 1, 2, 2, 1, 1, 2, 1)
NT = (((1,), (1,)), ((), ()))


def nt_dot(a, b, precision=None):
    return lax.dot_general(a, b, NT, precision=precision, preferred_element_type=jnp.float32)


def plain_dot(a, b, precision=None):
    return jnp.dot(a, b, precision=precision, preferred_element_type=jnp.float32)


def lane_masks():
    lane = lax.broadcasted_iota(jnp.int32, (1, HALF), 1)
    return (
        (lane < 64).astype(jnp.float32).astype(jnp.bfloat16),
        (lane >= 64).astype(jnp.float32).astype(jnp.bfloat16),
    )


def turned_rows(states, g):
    first = states[g // 4, 2 * lax.rem(g, 4)].astype(jnp.float32)
    second = states[g // 4, 2 * lax.rem(g, 4) + 1].astype(jnp.float32)
    return (
        jnp.concatenate([first[:8], second[:8]], axis=0).astype(jnp.bfloat16),
        jnp.concatenate([first[8:], second[8:]], axis=0).astype(jnp.bfloat16),
    )


def spread(one, two):
    low, high = lane_masks()
    blank = jnp.zeros((2 * STATE, HALF), jnp.bfloat16)
    top = jnp.concatenate([one * low, one * high], axis=0)
    bottom = jnp.concatenate([two * low, two * high], axis=0)
    return jnp.concatenate(
        [
            jnp.concatenate([top, blank], axis=1),
            jnp.concatenate([blank, bottom], axis=1),
        ],
        axis=0,
    )


def across(c, pair, carry, states, b_wide, xv, dyv, partial_x, to_end_s, from_start_s, store):
    cross_b, cross_c = carry
    groups = (2 * pair, 2 * pair + 1)
    lanes = [pl.ds(pl.multiple_of(g * LANES + HALF * c, HALF), HALF) for g in groups]
    state_one, grad_one = turned_rows(states, groups[0])
    state_two, grad_two = turned_rows(states, groups[1])
    state = spread(state_one, state_two)
    grad = spread(grad_one, grad_two)
    heads = slice(2 * c, 2 * c + 2)
    ends = jnp.concatenate([to_end_s[g][heads] for g in groups], axis=0)
    starts = jnp.concatenate([from_start_s[g][heads] for g in groups], axis=0)
    into = jnp.concatenate([b_wide * ends[k : k + 1, :] for k in range(4)], axis=0)
    term = plain_dot(jnp.transpose(into).astype(jnp.bfloat16), grad)
    for k in range(2):
        store(
            groups[k],
            lanes[k],
            (partial_x[:, lanes[k]] + term[:, HALF * k : HALF * k + HALF]).astype(jnp.bfloat16),
        )
    x = jnp.concatenate([xv[:, part] for part in lanes], axis=1)
    dy = jnp.concatenate([dyv[:, part] for part in lanes], axis=1)
    from_x = nt_dot(grad, x)
    from_dy = nt_dot(state, dy)
    for k in range(4):
        take = slice(STATE * k, STATE * k + STATE)
        cross_b += from_x[take] * ends[k : k + 1, :]
        cross_c += from_dy[take] * starts[k : k + 1, :]
    return cross_b, cross_c


def kernel(
    length_ref,
    skip_hbm,
    x_hbm,
    dy_hbm,
    dt_hbm,
    decay_hbm,
    b_hbm,
    c_hbm,
    gx_ref,
    cross_b_ref,
    cross_c_ref,
    xv,
    dyv,
    partial_x,
    to_end_s,
    from_start_s,
    b_out,
    late_states,
    skip_ref,
    dt_ref,
    decay_ref,
    b_ref,
    c_ref,
    row_s,
    col_s,
    cb_s,
    mix_s,
    parts_out,
    parts_in,
    ends_out,
    ends_in,
    inside,
    totals_out,
    totals_in,
    quad_out,
    quad_in,
    before_out,
    before_in,
    states_out,
    states_in,
    load_x_sem,
    load_dy_sem,
    load_sem,
    send_sem,
    recv_sem,
):
    me = lax.axis_index("seq")
    lane_of_batch = lax.axis_index("batch")

    my_z = me // ROWS
    my_x = lax.rem(me, ROWS)
    row_offsets = (2, 1, 3)
    column_offsets = (4, 3, 5, 2, 6, 1, 7)

    def row_peer(dx):
        return lax.rem(my_x + dx, ROWS)

    def column_peer(dz):
        return lax.rem(my_z + dz, COLUMNS)

    def row_device(dx):
        return (my_z * ROWS + row_peer(dx), lane_of_batch)

    def column_device(dz):
        return (column_peer(dz) * ROWS + my_x, lane_of_batch)

    small = [
        pltpu.make_async_copy(source, target, load_sem.at[i])
        for i, (source, target) in enumerate(
            (
                (decay_hbm, decay_ref),
                (dt_hbm, dt_ref),
                (b_hbm, b_ref),
                (c_hbm, c_ref),
                (skip_hbm, skip_ref),
            )
        )
    ]
    for copy in small:
        copy.start()

    quarters = [row_peer(dx) for dx in row_offsets + (0,)]
    loads_x, loads_dy = [], []
    for i, quarter in enumerate(quarters):
        part = pl.ds(pl.multiple_of(quarter * QUARTER, HALF), QUARTER)
        loads_x.append(pltpu.make_async_copy(x_hbm.at[0, :, part], xv.at[:, part], load_x_sem.at[i]))
        loads_dy.append(
            pltpu.make_async_copy(dy_hbm.at[0, :, part], dyv.at[:, part], load_dy_sem.at[i])
        )
    for i in range(LOAD_CHUNKS):
        loads_x[i].start()
        loads_dy[i].start()

    barrier = pltpu.get_barrier_semaphore()

    for dx in row_offsets:
        pl.semaphore_signal(barrier, inc=1, device_id=row_device(dx), device_id_type=MESH)
    for dz in column_offsets:
        pl.semaphore_signal(barrier, inc=1, device_id=column_device(dz), device_id_type=MESH)

    for copy in small:
        copy.wait()
    decay = decay_ref[0]
    dt = dt_ref[0]
    rows = lax.broadcasted_iota(jnp.int32, (SPAN, SPAN), 0)
    cols = lax.broadcasted_iota(jnp.int32, (SPAN, SPAN), 1)
    cum = plain_dot(decay, (rows <= cols).astype(jnp.float32), HIGHEST)
    from_start = jnp.exp(cum)
    to_end = dt * jnp.exp(cum[:, SPAN - 1 :] - cum)
    row_log = cum * LOG2E
    col_log = row_log - jnp.log(dt) * LOG2E
    for g in range(GROUPS):
        take = slice(g * HEADS_PER_GROUP, (g + 1) * HEADS_PER_GROUP)
        row_s[g, 0:HEADS_PER_GROUP, :] = row_log[take]
        col_s[g, 0:HEADS_PER_GROUP, :] = col_log[take]
        to_end_s[g, 0:HEADS_PER_GROUP, :] = to_end[take]
        from_start_s[g, 0:HEADS_PER_GROUP, :] = from_start[take]
    padded = jnp.concatenate([decay, jnp.zeros((32, SPAN), jnp.float32)], axis=0)
    total = nt_dot(jnp.ones((8, SPAN), jnp.float32), padded, HIGHEST)
    ends = jnp.exp(total[0:1])
    ends_high = ends.astype(jnp.bfloat16)
    rest = ends - ends_high.astype(jnp.float32)
    ends_mid = rest.astype(jnp.bfloat16)
    ends_low = rest - ends_mid.astype(jnp.float32)
    split_ends = jnp.concatenate(
        [
            ends_high.astype(jnp.float32),
            ends_mid.astype(jnp.float32),
            ends_low,
            jnp.zeros((13, HALF), jnp.float32),
        ],
        axis=0,
    ).astype(jnp.bfloat16)
    head_row = lax.broadcasted_iota(jnp.int32, (HALF, LANES), 0)
    lane_head = lax.broadcasted_iota(jnp.int32, (HALF, LANES), 1) // 64
    b_wide = b_ref[0].astype(jnp.float32)
    c_wide = c_ref[0].astype(jnp.float32)
    b_turned = jnp.transpose(b_wide).astype(jnp.bfloat16)
    cb_s[...] = plain_dot(b_turned, c_ref[0])
    mix_s[...] = jnp.zeros_like(mix_s)

    position = lax.broadcasted_iota(jnp.int32, (SPAN, 1), 0) + me * SPAN
    valid = (position < length_ref[0]).astype(jnp.float32).astype(jnp.bfloat16)
    low = lax.broadcasted_iota(jnp.int32, (STATE, HALF), 1) < 64

    def lanes_of(g):
        return pl.ds(pl.multiple_of(g * LANES, HALF), LANES)

    def per_head(wide, weights):
        return jnp.concatenate(
            [(wide * weights[k : k + 1, :]).astype(jnp.bfloat16) for k in range(HEADS_PER_GROUP)],
            axis=0,
        )

    def own_heads(product):
        pieces = []
        for k in range(3):
            block = product[32 * k : 32 * k + 32, HALF * k : HALF * k + HALF]
            pieces.append(jnp.where(low, block[:STATE], block[STATE:]))
        return jnp.concatenate(pieces, axis=1)

    def summary(g, carry):
        lanes = lanes_of(g)
        dy = dyv[:, lanes] * valid
        dyv[:, lanes] = dy
        state = own_heads(plain_dot(per_head(b_wide, to_end_s[g]), xv[:, lanes]))
        grad = own_heads(plain_dot(per_head(c_wide, from_start_s[g]), dy))
        for half in range(2):
            take = slice(8 * half, 8 * half + 8)
            both = jnp.concatenate([state[take], grad[take]], axis=0).astype(jnp.bfloat16)
            for c in range(CHUNKS):
                parts_out[c, g // 4, 2 * lax.rem(g, 4) + half] = both[:, HALF * c : HALF * c + HALF]
        pick = (head_row == lane_head + g * HEADS_PER_GROUP).astype(jnp.float32)
        wide = plain_dot(split_ends, pick.astype(jnp.bfloat16))
        ends_out[g // 4, :, pl.ds(pl.multiple_of(lax.rem(g, 4) * LANES, HALF), LANES)] = (
            wide[0:1] + wide[1:2] + wide[2:3]
        )
        return carry

    def remote(source, target, slot, device):
        return pltpu.make_async_remote_copy(
            src_ref=source,
            dst_ref=target,
            send_sem=send_sem.at[slot],
            recv_sem=recv_sem.at[slot],
            device_id=device,
            device_id_type=MESH,
        )

    def row_wait(out_ref, in_ref, slot):
        few = pl.ds(0, ROWS - 1)
        return remote(out_ref.at[few], in_ref.at[few], slot, row_device(1))

    def column_wait(out_ref, in_ref, slot):
        few = pl.ds(0, COLUMNS - 1)
        return remote(out_ref.at[few], in_ref.at[few], slot, column_device(1))

    def send_part(c, dx):
        remote(
            parts_out.at[c, row_peer(dx)], parts_in.at[c, my_x], c, row_device(dx)
        ).start()

    def send_parts(c):
        for dx in row_offsets:
            send_part(c, dx)

    for i, quarter in enumerate(quarters):
        loads_x[i].wait()
        loads_dy[i].wait()
        lax.fori_loop(
            0,
            2,
            lambda k, carry, first=4 * quarter: summary(
                first + 2 * k + 1, summary(first + 2 * k, carry)
            ),
            0,
        )
        if i == 0:
            pl.semaphore_wait(barrier, ROWS + COLUMNS - 2)
        if i < ROWS - 1:
            dx = row_offsets[i]
            remote(ends_out.at[quarter], ends_in.at[my_x], 12, row_device(dx)).start()
            send_part(0, dx)
    send_parts(1)
    for c in range(CHUNKS):
        parts_in[c, my_x] = parts_out[c, my_x]
    ends_in[my_x] = ends_out[my_x]

    causal = lax.broadcasted_iota(jnp.int32, (HALF, HALF), 0) <= lax.broadcasted_iota(
        jnp.int32, (HALF, HALF), 1
    )
    lane_row = lax.broadcasted_iota(jnp.int32, (1, HALF), 1)
    keep = lane_masks()

    def within(g, carry):
        turned = jnp.transpose(col_s[g])
        logs = row_s[g]
        mix_aa = jnp.zeros((HALF, HALF), jnp.float32)
        mix_ab = jnp.zeros((HALF, HALF), jnp.float32)
        mix_bb = jnp.zeros((HALF, HALF), jnp.float32)
        for pair in range(3):
            lanes = pl.ds(pl.multiple_of(g * LANES + pair * HALF, HALF), HALF)
            x = xv[:, lanes]
            dy = dyv[:, lanes]
            first = jnp.zeros((HALF, HALF), jnp.float32)
            second = jnp.zeros((HALF, HALF), jnp.float32)
            for side in range(2):
                k = 2 * pair + side
                dy_one = dy * keep[side]
                score_a = nt_dot(x[:HALF], dy_one)
                score_b = nt_dot(x[HALF:], dy_one[HALF:])
                gap_aa = logs[k : k + 1, :HALF] - turned[:HALF, k : k + 1]
                gap_ab = logs[k : k + 1, HALF:] - turned[:HALF, k : k + 1]
                gap_bb = logs[k : k + 1, HALF:] - turned[HALF:, k : k + 1]
                fade_aa = jnp.exp2(jnp.where(causal, gap_aa, -jnp.inf))
                fade_ab = jnp.exp2(gap_ab)
                fade_bb = jnp.exp2(jnp.where(causal, gap_bb, -jnp.inf))
                mix_aa += fade_aa * score_a[:, :HALF]
                mix_ab += fade_ab * score_a[:, HALF:]
                mix_bb += fade_bb * score_b
                kernel_a = jnp.concatenate(
                    [
                        (fade_aa * cb_s[:HALF, :HALF]).astype(jnp.bfloat16),
                        (fade_ab * cb_s[:HALF, HALF:]).astype(jnp.bfloat16),
                    ],
                    axis=1,
                )
                kernel_b = (fade_bb * cb_s[HALF:, HALF:]).astype(jnp.bfloat16)
                first += plain_dot(kernel_a, dy_one)
                second += plain_dot(kernel_b, dy_one[HALF:])
            skip = jnp.where(
                lane_row < 64,
                skip_ref[HEADS_PER_GROUP * g + 2 * pair],
                skip_ref[HEADS_PER_GROUP * g + 2 * pair + 1],
            )
            direct = skip * dy.astype(jnp.float32)
            partial_x[:HALF, lanes] = first + direct[:HALF]
            partial_x[HALF:, lanes] = second + direct[HALF:]
        mix_s[:HALF, :HALF] += mix_aa
        mix_s[:HALF, HALF:] += mix_ab
        mix_s[HALF:, HALF:] += mix_bb
        return carry

    fills = list(FILL)
    done = [0]

    def fill():
        count = fills.pop(0)
        lax.fori_loop(done[0], done[0] + count, within, 0)
        done[0] += count

    def decay_rows(z, c):
        lanes = slice(LANES * (z // 2) + HALF * c, LANES * (z // 2) + HALF * c + HALF)
        return [ends_in[x, :, lanes] for x in range(ROWS)]

    def join_row(c):
        row_wait(parts_out.at[c], parts_in.at[c], c).wait_recv()
        if c == 0:
            row_wait(ends_out, ends_in, 12).wait_recv()
            quad = ends_in[0] * ends_in[1] * ends_in[2] * ends_in[3]
            for k in range(4):
                quad_out[k] = quad[:, LANES * k : LANES * k + LANES]
        for z in range(COLUMNS):
            decays = decay_rows(z, c)
            parts = [parts_in[c, x, z].astype(jnp.float32) for x in range(ROWS)]
            state = jnp.zeros((8, HALF), jnp.float32)
            states = []
            for x in range(ROWS):
                states.append(state)
                state = decays[x] * state + parts[x][:8]
            grad = jnp.zeros((8, HALF), jnp.float32)
            grads = [None] * ROWS
            for x in reversed(range(ROWS)):
                grads[x] = grad
                grad = decays[x] * grad + parts[x][8:]
            totals_out[c, z] = jnp.concatenate([state, grad], axis=0).astype(jnp.bfloat16)
            for x in range(ROWS):
                inside[c, x, z] = jnp.concatenate([states[x], grads[x]], axis=0)
        if c == 0:
            for dz in column_offsets:
                remote(
                    quad_out.at[column_peer(dz) // 2], quad_in.at[my_z], 13, column_device(dz)
                ).start()
            quad_in[my_z] = quad_out[my_z // 2]
        for dz in column_offsets:
            remote(
                totals_out.at[c, column_peer(dz)],
                totals_in.at[c, my_z],
                3 + c,
                column_device(dz),
            ).start()
        totals_in[c, my_z] = totals_out[c, my_z]

    def scan_column(c):
        column_wait(totals_out.at[c], totals_in.at[c], 3 + c).wait_recv()
        if c == 0:
            column_wait(quad_in, quad_in, 13).wait_recv()
        decays = [quad_in[z, :, HALF * c : HALF * c + HALF] for z in range(COLUMNS)]
        parts = [totals_in[c, z].astype(jnp.float32) for z in range(COLUMNS)]
        state = jnp.zeros((8, HALF), jnp.float32)
        states = []
        for z in range(COLUMNS):
            states.append(state)
            state = decays[z] * state + parts[z][:8]
        grad = jnp.zeros((8, HALF), jnp.float32)
        for z in reversed(range(COLUMNS)):
            before_out[c, z] = jnp.concatenate([states[z], grad], axis=0).astype(jnp.bfloat16)
            grad = decays[z] * grad + parts[z][8:]
        for dz in column_offsets:
            remote(
                before_out.at[c, column_peer(dz)],
                before_in.at[c, my_z],
                6 + c,
                column_device(dz),
            ).start()
        before_in[c, my_z] = before_out[c, my_z]

    def finish_row(c):
        column_wait(before_out.at[c], before_in.at[c], 6 + c).wait_recv()
        for z in range(COLUMNS):
            decays = decay_rows(z, c)
            outside = before_in[c, z].astype(jnp.float32)
            state = outside[:8]
            states = []
            for x in range(ROWS):
                states.append(state)
                if x < ROWS - 1:
                    state = decays[x] * state
            grad = outside[8:]
            for x in reversed(range(ROWS)):
                entering = jnp.concatenate([states[x], grad], axis=0) + inside[c, x, z]
                states_out[c, x, z] = entering.astype(jnp.bfloat16)
                if x > 0:
                    grad = decays[x] * grad
        for dx in row_offsets:
            remote(
                states_out.at[c, row_peer(dx)], states_in.at[c, my_x], 9 + c, row_device(dx)
            ).start()
        states_in[c, my_x] = states_out[c, my_x]

    fill()
    send_parts(2)
    for stage in (join_row, scan_column, finish_row):
        for c in range(CHUNKS):
            fill()
            stage(c)
    fill()
    mixing = mix_s[...]
    base_b = nt_dot(c_wide, mixing, HIGHEST)
    base_c = plain_dot(b_wide, mixing, HIGHEST)

    def store(g, lanes, tile):
        gx_ref[0, :, lanes] = tile

    refs = (b_wide, xv, dyv, partial_x, to_end_s, from_start_s, store)
    crosses = (base_b, base_c)
    b_out[...] = b_ref[...]
    for c in range(CHUNKS - 1):
        row_wait(states_out.at[c], states_in.at[c], 9 + c).wait_recv()
        states = states_in.at[c]
        crosses = lax.fori_loop(
            0,
            GROUPS // 4,
            lambda two, carry, c=c, states=states: across(
                c, 2 * two + 1, across(c, 2 * two, carry, states, *refs), states, *refs
            ),
            crosses,
        )
    cross_b_ref[0], cross_c_ref[0] = crosses
    final = CHUNKS - 1
    row_wait(states_out.at[final], states_in.at[final], 9 + final).wait_recv()
    late_states[...] = states_in[final]

    for c in range(CHUNKS):
        row_wait(parts_out.at[c], parts_in.at[c], c).wait_send()
        column_wait(totals_out.at[c], totals_in.at[c], 3 + c).wait_send()
        column_wait(before_out.at[c], before_in.at[c], 6 + c).wait_send()
        row_wait(states_out.at[c], states_in.at[c], 9 + c).wait_send()
    row_wait(ends_out, ends_in, 12).wait_send()
    column_wait(quad_in, quad_in, 13).wait_send()


def finish(
    scale_b,
    scale_c,
    early_x,
    cross_b_ref,
    cross_c_ref,
    xv,
    dyv,
    partial_x,
    to_end_s,
    from_start_s,
    b_ref,
    states,
    gx_hbm,
    gb_hbm,
    gc_hbm,
    late_x,
    gb_v,
    gc_v,
    sem,
):
    final = CHUNKS - 1
    copies = []
    for g in range(GROUPS):
        part = pl.ds(g * LANES, HALF * final)
        copies.append(
            pltpu.make_async_copy(early_x.at[0, :, part], gx_hbm.at[0, :, part], sem.at[g])
        )
    for copy in copies:
        copy.start()

    def store(g, lanes, tile):
        late_x[g] = tile

    b_wide = b_ref[0].astype(jnp.float32)
    crosses = (cross_b_ref[0], cross_c_ref[0])
    for pair in range(GROUPS // 2):
        crosses = across(
            final,
            pair,
            crosses,
            states,
            b_wide,
            xv,
            dyv,
            partial_x,
            to_end_s,
            from_start_s,
            store,
        )
        for g in (2 * pair, 2 * pair + 1):
            part = pl.ds(g * LANES + HALF * final, HALF)
            copy = pltpu.make_async_copy(
                late_x.at[g], gx_hbm.at[0, :, part], sem.at[GROUPS + g]
            )
            copy.start()
            copies.append(copy)
    gb_v[0] = crosses[0] * scale_b
    gc_v[0] = crosses[1] * scale_c
    for k, (source, target) in enumerate(((gb_v, gb_hbm), (gc_v, gc_hbm))):
        copy = pltpu.make_async_copy(source, target, sem.at[2 * GROUPS + k])
        copy.start()
        copies.append(copy)
    for copy in copies:
        copy.wait()


def solution(mesh):
    def local(inputs, out_grad, step_size, log_decay, b_matrix, c_matrix, skip_gain, lengths):
        columns = inputs.shape[2]
        scale_b = 1.0 / math.sqrt(columns)
        scale_c = math.sqrt(STATE / (columns * PEERS * SPAN))
        vmem = pl.BlockSpec(memory_space=pltpu.VMEM)
        whole = pl.BlockSpec(memory_space=pltpu.HBM)
        f32, bf16 = jnp.float32, jnp.bfloat16
        shapes = (
            jax.ShapeDtypeStruct(inputs.shape, bf16),
            jax.ShapeDtypeStruct(b_matrix.shape, f32),
            jax.ShapeDtypeStruct(c_matrix.shape, f32),
        )
        rows = (SPAN, columns)
        between = (
            pltpu.VMEM(inputs.shape, bf16),
            pltpu.VMEM(b_matrix.shape, f32),
            pltpu.VMEM(c_matrix.shape, f32),
            pltpu.VMEM(rows, bf16),
            pltpu.VMEM(rows, bf16),
            pltpu.VMEM(rows, f32),
            pltpu.VMEM((GROUPS, 8, SPAN), f32),
            pltpu.VMEM((GROUPS, 8, SPAN), f32),
            pltpu.VMEM(b_matrix.shape, bf16),
            pltpu.VMEM((ROWS, COLUMNS, 16, HALF), bf16),
        )
        results = pl.pallas_call(
            kernel,
            out_shape=between,
            in_specs=[pl.BlockSpec(memory_space=pltpu.SMEM)] + [whole] * 7,
            out_specs=(vmem,) * len(between),
            scratch_shapes=[
                pltpu.SMEM((96,), f32),
                pltpu.VMEM((1, 96, SPAN), f32),
                pltpu.VMEM((1, 96, SPAN), f32),
                pltpu.VMEM((1, STATE, SPAN), bf16),
                pltpu.VMEM((1, STATE, SPAN), bf16),
                pltpu.VMEM((GROUPS, 8, SPAN), f32),
                pltpu.VMEM((GROUPS, 8, SPAN), f32),
                pltpu.VMEM((SPAN, SPAN), f32),
                pltpu.VMEM((SPAN, SPAN), f32),
                pltpu.VMEM((CHUNKS, ROWS, COLUMNS, 16, HALF), bf16),
                pltpu.VMEM((CHUNKS, ROWS, COLUMNS, 16, HALF), bf16),
                pltpu.VMEM((ROWS, 1, QUARTER), f32),
                pltpu.VMEM((ROWS, 1, QUARTER), f32),
                pltpu.VMEM((CHUNKS, ROWS, COLUMNS, 16, HALF), f32),
                pltpu.VMEM((CHUNKS, COLUMNS, 16, HALF), bf16),
                pltpu.VMEM((CHUNKS, COLUMNS, 16, HALF), bf16),
                pltpu.VMEM((4, 1, LANES), f32),
                pltpu.VMEM((COLUMNS, 1, LANES), f32),
                pltpu.VMEM((CHUNKS, COLUMNS, 16, HALF), bf16),
                pltpu.VMEM((CHUNKS, COLUMNS, 16, HALF), bf16),
                pltpu.VMEM((CHUNKS, ROWS, COLUMNS, 16, HALF), bf16),
                pltpu.VMEM((CHUNKS, ROWS, COLUMNS, 16, HALF), bf16),
                pltpu.SemaphoreType.DMA((LOAD_CHUNKS,)),
                pltpu.SemaphoreType.DMA((LOAD_CHUNKS,)),
                pltpu.SemaphoreType.DMA((5,)),
                pltpu.SemaphoreType.DMA((14,)),
                pltpu.SemaphoreType.DMA((14,)),
            ],
            compiler_params=pltpu.CompilerParams(
                collective_id=0, has_side_effects=True, vmem_limit_bytes=24 * 1024 * 1024
            ),
        )(
            lengths,
            *(
                pltpu.with_memory_space_constraint(operand, pltpu.HBM)
                for operand in (
                    skip_gain,
                    inputs,
                    out_grad,
                    step_size,
                    log_decay,
                    b_matrix,
                    c_matrix,
                )
            )
        )
        return pl.pallas_call(
            lambda *refs: finish(scale_b, scale_c, *refs),
            out_shape=shapes,
            in_specs=[vmem] * len(between),
            out_specs=(whole,) * 3,
            scratch_shapes=[
                pltpu.VMEM((GROUPS, SPAN, HALF), bf16),
                pltpu.VMEM(b_matrix.shape, f32),
                pltpu.VMEM(c_matrix.shape, f32),
                pltpu.SemaphoreType.DMA((2 * GROUPS + 2,)),
            ],
            compiler_params=pltpu.CompilerParams(vmem_limit_bytes=24 * 1024 * 1024),
        )(*(pltpu.with_memory_space_constraint(result, pltpu.VMEM) for result in results))

    return jax.shard_map(
        local,
        mesh=mesh,
        in_specs=(
            P("batch", "seq", None),
            P("batch", "seq", None),
            P("batch", None, "seq"),
            P("batch", None, "seq"),
            P("batch", None, "seq"),
            P("batch", None, "seq"),
            P(),
            P("batch"),
        ),
        out_specs=(P("batch", "seq", None), P("batch", None, "seq"), P("batch", None, "seq")),
        check_vma=False,
    )
```

```python
import math

import jax
import jax.numpy as jnp
from jax import lax
from jax.experimental import pallas as pl
from jax.experimental.pallas import tpu as pltpu
from jax.sharding import PartitionSpec as P

MESH = pl.DeviceIdType.MESH
HIGHEST = lax.Precision.HIGHEST
LOG2E = 1.4426950408889634
SPAN = 256
HALF = 128
STATE = 16
HEADS_PER_GROUP = 6
LANES = 384
GROUPS = 16
PEERS = 32
LOAD_CHUNKS = 4
ROWS = 4
COLUMNS = 8
CHUNKS = 3
QUARTER = 1536
WAIT_AFTER = 1
FILL = (2, 1, 1, 2, 1, 2, 2, 1, 1, 2, 1)
NT = (((1,), (1,)), ((), ()))


def nt_dot(a, b, precision=None):
    return lax.dot_general(a, b, NT, precision=precision, preferred_element_type=jnp.float32)


def plain_dot(a, b, precision=None):
    return jnp.dot(a, b, precision=precision, preferred_element_type=jnp.float32)


def lane_masks():
    lane = lax.broadcasted_iota(jnp.int32, (1, HALF), 1)
    return (
        (lane < 64).astype(jnp.float32).astype(jnp.bfloat16),
        (lane >= 64).astype(jnp.float32).astype(jnp.bfloat16),
    )


def turned_rows(states, g):
    first = states[g // 4, 2 * lax.rem(g, 4)].astype(jnp.float32)
    second = states[g // 4, 2 * lax.rem(g, 4) + 1].astype(jnp.float32)
    return (
        jnp.concatenate([first[:8], second[:8]], axis=0).astype(jnp.bfloat16),
        jnp.concatenate([first[8:], second[8:]], axis=0).astype(jnp.bfloat16),
    )


def spread(one, two):
    low, high = lane_masks()
    blank = jnp.zeros((2 * STATE, HALF), jnp.bfloat16)
    top = jnp.concatenate([one * low, one * high], axis=0)
    bottom = jnp.concatenate([two * low, two * high], axis=0)
    return jnp.concatenate(
        [
            jnp.concatenate([top, blank], axis=1),
            jnp.concatenate([blank, bottom], axis=1),
        ],
        axis=0,
    )


def across(c, pair, carry, states, b_wide, xv, dyv, partial_x, to_end_s, from_start_s, store):
    cross_b, cross_c = carry
    groups = (2 * pair, 2 * pair + 1)
    lanes = [pl.ds(pl.multiple_of(g * LANES + HALF * c, HALF), HALF) for g in groups]
    state_one, grad_one = turned_rows(states, groups[0])
    state_two, grad_two = turned_rows(states, groups[1])
    state = spread(state_one, state_two)
    grad = spread(grad_one, grad_two)
    heads = slice(2 * c, 2 * c + 2)
    ends = jnp.concatenate([to_end_s[g][heads] for g in groups], axis=0)
    starts = jnp.concatenate([from_start_s[g][heads] for g in groups], axis=0)
    into = jnp.concatenate([b_wide * ends[k : k + 1, :] for k in range(4)], axis=0)
    term = plain_dot(jnp.transpose(into).astype(jnp.bfloat16), grad)
    for k in range(2):
        store(
            groups[k],
            lanes[k],
            (partial_x[:, lanes[k]] + term[:, HALF * k : HALF * k + HALF]).astype(jnp.bfloat16),
        )
    x = jnp.concatenate([xv[:, part] for part in lanes], axis=1)
    dy = jnp.concatenate([dyv[:, part] for part in lanes], axis=1)
    from_x = nt_dot(grad, x)
    from_dy = nt_dot(state, dy)
    for k in range(4):
        take = slice(STATE * k, STATE * k + STATE)
        cross_b += from_x[take] * ends[k : k + 1, :]
        cross_c += from_dy[take] * starts[k : k + 1, :]
    return cross_b, cross_c


def kernel(
    length_ref,
    skip_hbm,
    x_hbm,
    dy_hbm,
    dt_hbm,
    decay_hbm,
    b_hbm,
    c_hbm,
    gx_ref,
    cross_b_ref,
    cross_c_ref,
    xv,
    dyv,
    partial_x,
    to_end_s,
    from_start_s,
    b_out,
    late_states,
    skip_ref,
    dt_ref,
    decay_ref,
    b_ref,
    c_ref,
    row_s,
    col_s,
    cb_s,
    mix_s,
    parts_out,
    parts_in,
    ends_out,
    ends_in,
    inside,
    totals_out,
    totals_in,
    quad_out,
    quad_in,
    before_out,
    before_in,
    states_out,
    states_in,
    load_x_sem,
    load_dy_sem,
    load_sem,
    send_sem,
    recv_sem,
):
    me = lax.axis_index("seq")
    lane_of_batch = lax.axis_index("batch")

    my_z = me // ROWS
    my_x = lax.rem(me, ROWS)
    row_offsets = (2, 1, 3)
    column_offsets = (4, 3, 5, 2, 6, 1, 7)

    def row_peer(dx):
        return lax.rem(my_x + dx, ROWS)

    def column_peer(dz):
        return lax.rem(my_z + dz, COLUMNS)

    def row_device(dx):
        return (my_z * ROWS + row_peer(dx), lane_of_batch)

    def column_device(dz):
        return (column_peer(dz) * ROWS + my_x, lane_of_batch)

    small = [
        pltpu.make_async_copy(source, target, load_sem.at[i])
        for i, (source, target) in enumerate(
            (
                (decay_hbm, decay_ref),
                (dt_hbm, dt_ref),
                (b_hbm, b_ref),
                (c_hbm, c_ref),
                (skip_hbm, skip_ref),
            )
        )
    ]
    for copy in small:
        copy.start()

    quarters = [row_peer(dx) for dx in row_offsets + (0,)]
    loads_x, loads_dy = [], []
    for i, quarter in enumerate(quarters):
        part = pl.ds(pl.multiple_of(quarter * QUARTER, HALF), QUARTER)
        loads_x.append(pltpu.make_async_copy(x_hbm.at[0, :, part], xv.at[:, part], load_x_sem.at[i]))
        loads_dy.append(
            pltpu.make_async_copy(dy_hbm.at[0, :, part], dyv.at[:, part], load_dy_sem.at[i])
        )
    for i in range(LOAD_CHUNKS):
        loads_x[i].start()
        loads_dy[i].start()

    barrier = pltpu.get_barrier_semaphore()

    for dx in row_offsets:
        pl.semaphore_signal(barrier, inc=1, device_id=row_device(dx), device_id_type=MESH)
    for dz in column_offsets:
        pl.semaphore_signal(barrier, inc=1, device_id=column_device(dz), device_id_type=MESH)

    for copy in small:
        copy.wait()
    decay = decay_ref[0]
    dt = dt_ref[0]
    rows = lax.broadcasted_iota(jnp.int32, (SPAN, SPAN), 0)
    cols = lax.broadcasted_iota(jnp.int32, (SPAN, SPAN), 1)
    cum = plain_dot(decay, (rows <= cols).astype(jnp.float32), HIGHEST)
    from_start = jnp.exp(cum)
    to_end = dt * jnp.exp(cum[:, SPAN - 1 :] - cum)
    row_log = cum * LOG2E
    col_log = row_log - jnp.log(dt) * LOG2E
    for g in range(GROUPS):
        take = slice(g * HEADS_PER_GROUP, (g + 1) * HEADS_PER_GROUP)
        row_s[g, 0:HEADS_PER_GROUP, :] = row_log[take]
        col_s[g, 0:HEADS_PER_GROUP, :] = col_log[take]
        to_end_s[g, 0:HEADS_PER_GROUP, :] = to_end[take]
        from_start_s[g, 0:HEADS_PER_GROUP, :] = from_start[take]
    padded = jnp.concatenate([decay, jnp.zeros((32, SPAN), jnp.float32)], axis=0)
    total = nt_dot(jnp.ones((8, SPAN), jnp.float32), padded, HIGHEST)
    ends = jnp.exp(total[0:1])
    ends_high = ends.astype(jnp.bfloat16)
    rest = ends - ends_high.astype(jnp.float32)
    ends_mid = rest.astype(jnp.bfloat16)
    ends_low = rest - ends_mid.astype(jnp.float32)
    split_ends = jnp.concatenate(
        [
            ends_high.astype(jnp.float32),
            ends_mid.astype(jnp.float32),
            ends_low,
            jnp.zeros((13, HALF), jnp.float32),
        ],
        axis=0,
    ).astype(jnp.bfloat16)
    head_row = lax.broadcasted_iota(jnp.int32, (HALF, LANES), 0)
    lane_head = lax.broadcasted_iota(jnp.int32, (HALF, LANES), 1) // 64
    b_wide = b_ref[0].astype(jnp.float32)
    c_wide = c_ref[0].astype(jnp.float32)
    b_turned = jnp.transpose(b_wide).astype(jnp.bfloat16)
    cb_s[...] = plain_dot(b_turned, c_ref[0])
    mix_s[...] = jnp.zeros_like(mix_s)

    position = lax.broadcasted_iota(jnp.int32, (SPAN, 1), 0) + me * SPAN
    valid = (position < length_ref[0]).astype(jnp.float32).astype(jnp.bfloat16)
    low = lax.broadcasted_iota(jnp.int32, (STATE, HALF), 1) < 64

    def lanes_of(g):
        return pl.ds(pl.multiple_of(g * LANES, HALF), LANES)

    def per_head(wide, weights):
        return jnp.concatenate(
            [(wide * weights[k : k + 1, :]).astype(jnp.bfloat16) for k in range(HEADS_PER_GROUP)],
            axis=0,
        )

    def own_heads(product):
        pieces = []
        for k in range(3):
            block = product[32 * k : 32 * k + 32, HALF * k : HALF * k + HALF]
            pieces.append(jnp.where(low, block[:STATE], block[STATE:]))
        return jnp.concatenate(pieces, axis=1)

    def summary(g, carry):
        lanes = lanes_of(g)
        dy = dyv[:, lanes] * valid
        dyv[:, lanes] = dy
        state = own_heads(plain_dot(per_head(b_wide, to_end_s[g]), xv[:, lanes]))
        grad = own_heads(plain_dot(per_head(c_wide, from_start_s[g]), dy))
        for half in range(2):
            take = slice(8 * half, 8 * half + 8)
            both = jnp.concatenate([state[take], grad[take]], axis=0).astype(jnp.bfloat16)
            for c in range(CHUNKS):
                parts_out[c, g // 4, 2 * lax.rem(g, 4) + half] = both[:, HALF * c : HALF * c + HALF]
        pick = (head_row == lane_head + g * HEADS_PER_GROUP).astype(jnp.float32)
        wide = plain_dot(split_ends, pick.astype(jnp.bfloat16))
        ends_out[g // 4, :, pl.ds(pl.multiple_of(lax.rem(g, 4) * LANES, HALF), LANES)] = (
            wide[0:1] + wide[1:2] + wide[2:3]
        )
        return carry

    def remote(source, target, slot, device):
        return pltpu.make_async_remote_copy(
            src_ref=source,
            dst_ref=target,
            send_sem=send_sem.at[slot],
            recv_sem=recv_sem.at[slot],
            device_id=device,
            device_id_type=MESH,
        )

    def row_wait(out_ref, in_ref, slot):
        few = pl.ds(0, ROWS - 1)
        return remote(out_ref.at[few], in_ref.at[few], slot, row_device(1))

    def column_wait(out_ref, in_ref, slot):
        few = pl.ds(0, COLUMNS - 1)
        return remote(out_ref.at[few], in_ref.at[few], slot, column_device(1))

    def send_part(c, dx):
        remote(
            parts_out.at[c, row_peer(dx)], parts_in.at[c, my_x], c, row_device(dx)
        ).start()

    def send_parts(c):
        for dx in row_offsets:
            send_part(c, dx)

    for i, quarter in enumerate(quarters):
        loads_x[i].wait()
        loads_dy[i].wait()
        lax.fori_loop(
            0,
            2,
            lambda k, carry, first=4 * quarter: summary(
                first + 2 * k + 1, summary(first + 2 * k, carry)
            ),
            0,
        )
        if i == WAIT_AFTER:
            pl.semaphore_wait(barrier, ROWS + COLUMNS - 2)
            ready = row_offsets[: i + 1]
        else:
            ready = row_offsets[i : i + 1] if i > WAIT_AFTER else ()
        for dx in ready:
            remote(ends_out.at[row_peer(dx)], ends_in.at[my_x], 12, row_device(dx)).start()
            send_part(0, dx)
    send_parts(1)
    for c in range(CHUNKS):
        parts_in[c, my_x] = parts_out[c, my_x]
    ends_in[my_x] = ends_out[my_x]

    causal = lax.broadcasted_iota(jnp.int32, (HALF, HALF), 0) <= lax.broadcasted_iota(
        jnp.int32, (HALF, HALF), 1
    )
    lane_row = lax.broadcasted_iota(jnp.int32, (1, HALF), 1)
    keep = lane_masks()

    def within(g, carry):
        turned = jnp.transpose(col_s[g])
        logs = row_s[g]
        mix_aa = jnp.zeros((HALF, HALF), jnp.float32)
        mix_ab = jnp.zeros((HALF, HALF), jnp.float32)
        mix_bb = jnp.zeros((HALF, HALF), jnp.float32)
        for pair in range(3):
            lanes = pl.ds(pl.multiple_of(g * LANES + pair * HALF, HALF), HALF)
            x = xv[:, lanes]
            dy = dyv[:, lanes]
            first = jnp.zeros((HALF, HALF), jnp.float32)
            second = jnp.zeros((HALF, HALF), jnp.float32)
            for side in range(2):
                k = 2 * pair + side
                dy_one = dy * keep[side]
                score_a = nt_dot(x[:HALF], dy_one)
                score_b = nt_dot(x[HALF:], dy_one[HALF:])
                gap_aa = logs[k : k + 1, :HALF] - turned[:HALF, k : k + 1]
                gap_ab = logs[k : k + 1, HALF:] - turned[:HALF, k : k + 1]
                gap_bb = logs[k : k + 1, HALF:] - turned[HALF:, k : k + 1]
                fade_aa = jnp.exp2(jnp.where(causal, gap_aa, -jnp.inf))
                fade_ab = jnp.exp2(gap_ab)
                fade_bb = jnp.exp2(jnp.where(causal, gap_bb, -jnp.inf))
                mix_aa += fade_aa * score_a[:, :HALF]
                mix_ab += fade_ab * score_a[:, HALF:]
                mix_bb += fade_bb * score_b
                kernel_a = jnp.concatenate(
                    [
                        (fade_aa * cb_s[:HALF, :HALF]).astype(jnp.bfloat16),
                        (fade_ab * cb_s[:HALF, HALF:]).astype(jnp.bfloat16),
                    ],
                    axis=1,
                )
                kernel_b = (fade_bb * cb_s[HALF:, HALF:]).astype(jnp.bfloat16)
                first += plain_dot(kernel_a, dy_one)
                second += plain_dot(kernel_b, dy_one[HALF:])
            skip = jnp.where(
                lane_row < 64,
                skip_ref[HEADS_PER_GROUP * g + 2 * pair],
                skip_ref[HEADS_PER_GROUP * g + 2 * pair + 1],
            )
            direct = skip * dy.astype(jnp.float32)
            partial_x[:HALF, lanes] = first + direct[:HALF]
            partial_x[HALF:, lanes] = second + direct[HALF:]
        mix_s[:HALF, :HALF] += mix_aa
        mix_s[:HALF, HALF:] += mix_ab
        mix_s[HALF:, HALF:] += mix_bb
        return carry

    fills = list(FILL)
    done = [0]

    def fill():
        count = fills.pop(0)
        lax.fori_loop(done[0], done[0] + count, within, 0)
        done[0] += count

    def decay_rows(z, c):
        lanes = slice(LANES * (z // 2) + HALF * c, LANES * (z // 2) + HALF * c + HALF)
        return [ends_in[x, :, lanes] for x in range(ROWS)]

    def join_row(c):
        row_wait(parts_out.at[c], parts_in.at[c], c).wait_recv()
        if c == 0:
            row_wait(ends_out, ends_in, 12).wait_recv()
            quad = ends_in[0] * ends_in[1] * ends_in[2] * ends_in[3]
            for k in range(4):
                quad_out[k] = quad[:, LANES * k : LANES * k + LANES]
        for z in range(COLUMNS):
            decays = decay_rows(z, c)
            parts = [parts_in[c, x, z].astype(jnp.float32) for x in range(ROWS)]
            state = jnp.zeros((8, HALF), jnp.float32)
            states = []
            for x in range(ROWS):
                states.append(state)
                state = decays[x] * state + parts[x][:8]
            grad = jnp.zeros((8, HALF), jnp.float32)
            grads = [None] * ROWS
            for x in reversed(range(ROWS)):
                grads[x] = grad
                grad = decays[x] * grad + parts[x][8:]
            totals_out[c, z] = jnp.concatenate([state, grad], axis=0).astype(jnp.bfloat16)
            for x in range(ROWS):
                inside[c, x, z] = jnp.concatenate([states[x], grads[x]], axis=0)
        if c == 0:
            for dz in column_offsets:
                remote(
                    quad_out.at[column_peer(dz) // 2], quad_in.at[my_z], 13, column_device(dz)
                ).start()
            quad_in[my_z] = quad_out[my_z // 2]
        for dz in column_offsets:
            remote(
                totals_out.at[c, column_peer(dz)],
                totals_in.at[c, my_z],
                3 + c,
                column_device(dz),
            ).start()
        totals_in[c, my_z] = totals_out[c, my_z]

    def scan_column(c):
        column_wait(totals_out.at[c], totals_in.at[c], 3 + c).wait_recv()
        if c == 0:
            column_wait(quad_in, quad_in, 13).wait_recv()
        decays = [quad_in[z, :, HALF * c : HALF * c + HALF] for z in range(COLUMNS)]
        parts = [totals_in[c, z].astype(jnp.float32) for z in range(COLUMNS)]
        state = jnp.zeros((8, HALF), jnp.float32)
        states = []
        for z in range(COLUMNS):
            states.append(state)
            state = decays[z] * state + parts[z][:8]
        grad = jnp.zeros((8, HALF), jnp.float32)
        for z in reversed(range(COLUMNS)):
            before_out[c, z] = jnp.concatenate([states[z], grad], axis=0).astype(jnp.bfloat16)
            grad = decays[z] * grad + parts[z][8:]
        for dz in column_offsets:
            remote(
                before_out.at[c, column_peer(dz)],
                before_in.at[c, my_z],
                6 + c,
                column_device(dz),
            ).start()
        before_in[c, my_z] = before_out[c, my_z]

    def finish_row(c):
        column_wait(before_out.at[c], before_in.at[c], 6 + c).wait_recv()
        for z in range(COLUMNS):
            decays = decay_rows(z, c)
            outside = before_in[c, z].astype(jnp.float32)
            state = outside[:8]
            states = []
            for x in range(ROWS):
                states.append(state)
                if x < ROWS - 1:
                    state = decays[x] * state
            grad = outside[8:]
            for x in reversed(range(ROWS)):
                entering = jnp.concatenate([states[x], grad], axis=0) + inside[c, x, z]
                states_out[c, x, z] = entering.astype(jnp.bfloat16)
                if x > 0:
                    grad = decays[x] * grad
        for dx in row_offsets:
            remote(
                states_out.at[c, row_peer(dx)], states_in.at[c, my_x], 9 + c, row_device(dx)
            ).start()
        states_in[c, my_x] = states_out[c, my_x]

    fill()
    send_parts(2)
    for stage in (join_row, scan_column, finish_row):
        for c in range(CHUNKS):
            fill()
            stage(c)
    fill()
    mixing = mix_s[...]
    base_b = nt_dot(c_wide, mixing, HIGHEST)
    base_c = plain_dot(b_wide, mixing, HIGHEST)

    def store(g, lanes, tile):
        gx_ref[0, :, lanes] = tile

    refs = (b_wide, xv, dyv, partial_x, to_end_s, from_start_s, store)
    crosses = (base_b, base_c)
    b_out[...] = b_ref[...]
    for c in range(CHUNKS - 1):
        row_wait(states_out.at[c], states_in.at[c], 9 + c).wait_recv()
        states = states_in.at[c]
        crosses = lax.fori_loop(
            0,
            GROUPS // 4,
            lambda two, carry, c=c, states=states: across(
                c, 2 * two + 1, across(c, 2 * two, carry, states, *refs), states, *refs
            ),
            crosses,
        )
    cross_b_ref[0], cross_c_ref[0] = crosses
    final = CHUNKS - 1
    row_wait(states_out.at[final], states_in.at[final], 9 + final).wait_recv()
    late_states[...] = states_in[final]

    for c in range(CHUNKS):
        row_wait(parts_out.at[c], parts_in.at[c], c).wait_send()
        column_wait(totals_out.at[c], totals_in.at[c], 3 + c).wait_send()
        column_wait(before_out.at[c], before_in.at[c], 6 + c).wait_send()
        row_wait(states_out.at[c], states_in.at[c], 9 + c).wait_send()
    row_wait(ends_out, ends_in, 12).wait_send()
    column_wait(quad_in, quad_in, 13).wait_send()


def finish(
    scale_b,
    scale_c,
    early_x,
    cross_b_ref,
    cross_c_ref,
    xv,
    dyv,
    partial_x,
    to_end_s,
    from_start_s,
    b_ref,
    states,
    gx_hbm,
    gb_hbm,
    gc_hbm,
    late_x,
    gb_v,
    gc_v,
    sem,
):
    final = CHUNKS - 1
    copies = []
    for g in range(GROUPS):
        part = pl.ds(g * LANES, HALF * final)
        copies.append(
            pltpu.make_async_copy(early_x.at[0, :, part], gx_hbm.at[0, :, part], sem.at[g])
        )
    for copy in copies:
        copy.start()

    def store(g, lanes, tile):
        late_x[g] = tile

    b_wide = b_ref[0].astype(jnp.float32)
    crosses = (cross_b_ref[0], cross_c_ref[0])
    for pair in range(GROUPS // 2):
        crosses = across(
            final,
            pair,
            crosses,
            states,
            b_wide,
            xv,
            dyv,
            partial_x,
            to_end_s,
            from_start_s,
            store,
        )
        for g in (2 * pair, 2 * pair + 1):
            part = pl.ds(g * LANES + HALF * final, HALF)
            copy = pltpu.make_async_copy(
                late_x.at[g], gx_hbm.at[0, :, part], sem.at[GROUPS + g]
            )
            copy.start()
            copies.append(copy)
    gb_v[0] = crosses[0] * scale_b
    gc_v[0] = crosses[1] * scale_c
    for k, (source, target) in enumerate(((gb_v, gb_hbm), (gc_v, gc_hbm))):
        copy = pltpu.make_async_copy(source, target, sem.at[2 * GROUPS + k])
        copy.start()
        copies.append(copy)
    for copy in copies:
        copy.wait()


def solution(mesh):
    def local(inputs, out_grad, step_size, log_decay, b_matrix, c_matrix, skip_gain, lengths):
        columns = inputs.shape[2]
        scale_b = 1.0 / math.sqrt(columns)
        scale_c = math.sqrt(STATE / (columns * PEERS * SPAN))
        vmem = pl.BlockSpec(memory_space=pltpu.VMEM)
        whole = pl.BlockSpec(memory_space=pltpu.HBM)
        f32, bf16 = jnp.float32, jnp.bfloat16
        shapes = (
            jax.ShapeDtypeStruct(inputs.shape, bf16),
            jax.ShapeDtypeStruct(b_matrix.shape, f32),
            jax.ShapeDtypeStruct(c_matrix.shape, f32),
        )
        rows = (SPAN, columns)
        between = (
            pltpu.VMEM(inputs.shape, bf16),
            pltpu.VMEM(b_matrix.shape, f32),
            pltpu.VMEM(c_matrix.shape, f32),
            pltpu.VMEM(rows, bf16),
            pltpu.VMEM(rows, bf16),
            pltpu.VMEM(rows, f32),
            pltpu.VMEM((GROUPS, 8, SPAN), f32),
            pltpu.VMEM((GROUPS, 8, SPAN), f32),
            pltpu.VMEM(b_matrix.shape, bf16),
            pltpu.VMEM((ROWS, COLUMNS, 16, HALF), bf16),
        )
        results = pl.pallas_call(
            kernel,
            out_shape=between,
            in_specs=[pl.BlockSpec(memory_space=pltpu.SMEM)] + [whole] * 7,
            out_specs=(vmem,) * len(between),
            scratch_shapes=[
                pltpu.SMEM((96,), f32),
                pltpu.VMEM((1, 96, SPAN), f32),
                pltpu.VMEM((1, 96, SPAN), f32),
                pltpu.VMEM((1, STATE, SPAN), bf16),
                pltpu.VMEM((1, STATE, SPAN), bf16),
                pltpu.VMEM((GROUPS, 8, SPAN), f32),
                pltpu.VMEM((GROUPS, 8, SPAN), f32),
                pltpu.VMEM((SPAN, SPAN), f32),
                pltpu.VMEM((SPAN, SPAN), f32),
                pltpu.VMEM((CHUNKS, ROWS, COLUMNS, 16, HALF), bf16),
                pltpu.VMEM((CHUNKS, ROWS, COLUMNS, 16, HALF), bf16),
                pltpu.VMEM((ROWS, 1, QUARTER), f32),
                pltpu.VMEM((ROWS, 1, QUARTER), f32),
                pltpu.VMEM((CHUNKS, ROWS, COLUMNS, 16, HALF), f32),
                pltpu.VMEM((CHUNKS, COLUMNS, 16, HALF), bf16),
                pltpu.VMEM((CHUNKS, COLUMNS, 16, HALF), bf16),
                pltpu.VMEM((4, 1, LANES), f32),
                pltpu.VMEM((COLUMNS, 1, LANES), f32),
                pltpu.VMEM((CHUNKS, COLUMNS, 16, HALF), bf16),
                pltpu.VMEM((CHUNKS, COLUMNS, 16, HALF), bf16),
                pltpu.VMEM((CHUNKS, ROWS, COLUMNS, 16, HALF), bf16),
                pltpu.VMEM((CHUNKS, ROWS, COLUMNS, 16, HALF), bf16),
                pltpu.SemaphoreType.DMA((LOAD_CHUNKS,)),
                pltpu.SemaphoreType.DMA((LOAD_CHUNKS,)),
                pltpu.SemaphoreType.DMA((5,)),
                pltpu.SemaphoreType.DMA((14,)),
                pltpu.SemaphoreType.DMA((14,)),
            ],
            compiler_params=pltpu.CompilerParams(
                collective_id=0, has_side_effects=True, vmem_limit_bytes=24 * 1024 * 1024
            ),
        )(
            lengths,
            *(
                pltpu.with_memory_space_constraint(operand, pltpu.HBM)
                for operand in (
                    skip_gain,
                    inputs,
                    out_grad,
                    step_size,
                    log_decay,
                    b_matrix,
                    c_matrix,
                )
            )
        )
        return pl.pallas_call(
            lambda *refs: finish(scale_b, scale_c, *refs),
            out_shape=shapes,
            in_specs=[vmem] * len(between),
            out_specs=(whole,) * 3,
            scratch_shapes=[
                pltpu.VMEM((GROUPS, SPAN, HALF), bf16),
                pltpu.VMEM(b_matrix.shape, f32),
                pltpu.VMEM(c_matrix.shape, f32),
                pltpu.SemaphoreType.DMA((2 * GROUPS + 2,)),
            ],
            compiler_params=pltpu.CompilerParams(vmem_limit_bytes=24 * 1024 * 1024),
        )(*(pltpu.with_memory_space_constraint(result, pltpu.VMEM) for result in results))

    return jax.shard_map(
        local,
        mesh=mesh,
        in_specs=(
            P("batch", "seq", None),
            P("batch", "seq", None),
            P("batch", None, "seq"),
            P("batch", None, "seq"),
            P("batch", None, "seq"),
            P("batch", None, "seq"),
            P(),
            P("batch"),
        ),
        out_specs=(P("batch", "seq", None), P("batch", None, "seq"), P("batch", None, "seq")),
        check_vma=False,
    )
```
